128 devices in a mesh: row: 8 (over y, x_lo), col: 16 (over x_hi, z, core).
Axes of the slice: x: 4 (x_hi: 2, x_lo: 2; x = x_hi * 2 + x_lo), y: 4, z: 4, core: 2. Of those that a mesh axis runs over, the one named last changes fastest.
Arguments:
- patches: bfloat16 [64, 128, 768], P('row', 'col'), may hold values from -6 to 6
- w_patch: bfloat16 [768, 6144], replicated, may hold values from -0.21875 to 0.21875
- patch_bias: bfloat16 [6144], replicated, may hold values from -5 to 5
- ln_gain: bfloat16 [6144], replicated, may hold values from 0.5 to 1.5
- w_qkv: bfloat16 [6144, 3, 48, 128], P(None, None, 'col'), may hold values from -1 to 1
- qk_gain: float32 [2, 48, 128], P(None, 'col'), may hold values from 0 to 6, as said below
- w_out: bfloat16 [48, 128, 6144], P('col', None, 'row'), may hold values from -0.078125 to 0.078125
Outputs:
- attn_branch: bfloat16 [8192, 6144], P(('row', 'col'))
The draws below stay inside these ranges and needn't reach their ends.
Inputs may be any that keep to these rules, and one draw needn't show every extreme that they name: `qk_gain`: positive gains.
All inputs are finite; a program needn't handle non-finite values.
Results may differ from the reference program's by a relative error of at most 0.015.
Values may be sent and summed in bfloat16 or wider, within the bound.
A program may use at most 320 MiB of HBM per device.

```python
import math
import jax
import jax.numpy as jnp
from jax import lax

D = 6144
H = 48
HD = 128
PATCH_IN = 768
GW = 128
GH = 64
N_COL = 16


def draw_patches(key, part):
    key_one = jax.random.fold_in(key, 0)
    result = jnp.clip(jax.random.normal(key_one, (GH, GW, PATCH_IN), jnp.float32), -6.0, 6.0)
    return result.astype(jnp.bfloat16)


def draw_w_qkv(key, part):
    key_weight = jax.random.fold_in(key, 0)
    raw_draw = jnp.clip(jax.random.normal(key_weight, (D, 3, H, HD), jnp.float32), -6.0, 6.0) * D ** (-0.5)
    return raw_draw.astype(jnp.bfloat16)


def draw_qk_gain(key, part):
    key_head, key_dim = jax.random.split(key, 2)
    head_scale = jnp.exp(jax.random.uniform(key_head, (2, H, 1), jnp.float32, 0.5, 1.5))
    gains = head_scale * (1.0 + 0.1 * jnp.clip(jax.random.normal(key_dim, (2, H, HD), jnp.float32), -3.0, 3.0))
    return gains.astype(jnp.float32)


def shard_levels(key, extent, cuts, smallest, largest):
    def one(dim, shards_of):
        heights = jax.random.uniform(jax.random.fold_in(jax.random.fold_in(key, 6), dim), (shards_of,), jnp.float32, smallest / len(cuts), largest / len(cuts))
        return jnp.repeat(jnp.exp(heights), extent[dim] // shards_of).reshape((-1,) + (1,) * (len(extent) - dim - 1))

    gain = one(*cuts[0])
    for cut in cuts[1:]:
        gain = gain * one(*cut)
    return gain


def centred(stream_key, dims, spread, limit, pieces=(), held_as=jnp.bfloat16):
    entries = jax.random.normal(stream_key, dims, jnp.float32) * spread
    if len(pieces) > 0:
        entries = shard_levels(stream_key, dims, pieces, -0.22, 0.18) * entries
    return jnp.clip(entries, min=-limit, max=limit).astype(held_as)


def setup_inputs(seed: int = 0) -> dict:
    arg_keys = jax.random.split(jax.random.key(seed), 8)
    patches = draw_patches(jax.random.fold_in(arg_keys[7], 71), 0)
    w_patch = centred(arg_keys[1], (PATCH_IN, D), PATCH_IN ** -0.5, 0.21875)
    patch_bias = centred(arg_keys[2], (D,), 1.0, 5.0)
    ln_gain = jnp.clip(1.0 + 0.1 * jax.random.normal(arg_keys[3], (D,), jnp.float32), 0.5, 1.5).astype(jnp.bfloat16)
    w_qkv = draw_w_qkv(jax.random.fold_in(arg_keys[7], 71), 0)
    qk_gain = draw_qk_gain(jax.random.fold_in(arg_keys[7], 71), 0)
    w_out = centred(arg_keys[6], (H, HD, D), (H * HD) ** -0.5, 0.078125, ((0, 16), (2, 8)))
    return dict(patches=patches, w_patch=w_patch, patch_bias=patch_bias, ln_gain=ln_gain, w_qkv=w_qkv, qk_gain=qk_gain, w_out=w_out)


NORM_EPS = 1e-06

def sincos_table(row_ids, col_ids, model_width):
    quarter = model_width // 4
    frequency = 1.0 / 10000.0 ** (jnp.arange(quarter, dtype=jnp.float32) / quarter)
    row_angle = row_ids.astype(jnp.float32)[:, None] * frequency[None, :]
    col_angle = col_ids.astype(jnp.float32)[:, None] * frequency[None, :]
    return jnp.concatenate([jnp.sin(row_angle), jnp.cos(row_angle), jnp.sin(col_angle), jnp.cos(col_angle)], axis=1)

def layer_norm(values, gain_row):
    mean_val = lax.optimization_barrier(jnp.mean(values, axis=-1, keepdims=True))
    centered = values - mean_val
    variance = lax.optimization_barrier(jnp.mean(centered * centered, axis=-1, keepdims=True))
    return centered * lax.rsqrt(variance + NORM_EPS) * gain_row

def reference(patches, w_patch, patch_bias, ln_gain, w_qkv, qk_gain, w_out):
    token_count = GH * GW
    token_ids = jnp.arange(token_count, dtype=jnp.int32)
    flat_pixels = patches.reshape(token_count, PATCH_IN)
    embedded = jnp.dot(flat_pixels, w_patch, preferred_element_type=jnp.float32)
    embedded = embedded + patch_bias.astype(jnp.float32)[None, :] + sincos_table(token_ids // GW, token_ids % GW, D)
    normed = layer_norm(embedded, ln_gain.astype(jnp.float32)).astype(jnp.bfloat16)
    projected = jnp.dot(normed, w_qkv.reshape(D, 3 * H * HD), preferred_element_type=jnp.float32)
    projected = projected.reshape(token_count, 3, H, HD)
    queries = layer_norm(projected[:, 0], qk_gain[0]).astype(jnp.bfloat16)
    keys_all = layer_norm(projected[:, 1], qk_gain[1]).astype(jnp.bfloat16)
    values_all = projected[:, 2].astype(jnp.bfloat16)
    scale_factor = 1.0 / math.sqrt(HD)
    query_block = math.gcd(token_count, 1024)

    def one_head(head_args):
        head_q, head_k, head_v = head_args

        def one_block(block_q):
            scores = jnp.dot(block_q, head_k.T, preferred_element_type=jnp.float32) * scale_factor
            row_peak = lax.optimization_barrier(jnp.max(scores, axis=1, keepdims=True))
            exponent = jnp.exp(scores - row_peak)
            weight_sum = lax.optimization_barrier(jnp.sum(exponent, axis=1, keepdims=True))
            mixed_sum = jnp.dot(exponent.astype(jnp.bfloat16), head_v, preferred_element_type=jnp.float32)
            return (mixed_sum / weight_sum).astype(jnp.bfloat16)
        blocks = lax.map(one_block, head_q.reshape(token_count // query_block, query_block, HD))
        return blocks.reshape(token_count, HD)
    context = lax.map(one_head, (queries.transpose(1, 0, 2), keys_all.transpose(1, 0, 2), values_all.transpose(1, 0, 2)))
    context = context.transpose(1, 0, 2).reshape(token_count, H * HD)
    grouped_ctx = context.reshape(token_count, N_COL, H // N_COL * HD).transpose(1, 0, 2)
    grouped_w = w_out.reshape(N_COL, H // N_COL * HD, D)

    def add_group(running, group_args):
        group_ctx, group_w = group_args
        partial_term = jnp.dot(group_ctx, group_w, preferred_element_type=jnp.float32)
        rounded = lax.optimization_barrier(partial_term.astype(jnp.bfloat16))
        return (running + rounded.astype(jnp.float32), None)
    summed, unused = lax.scan(add_group, jnp.zeros((token_count, D), jnp.float32), (grouped_ctx, grouped_w))
    return summed.astype(jnp.bfloat16)
```

```python
import functools
import math

import numpy as np
import jax
import jax.numpy as jnp
from jax import lax
from jax.experimental import pallas as pl
from jax.experimental.pallas import tpu as pltpu
from jax.sharding import PartitionSpec as P

NORM_EPS = 1e-06
MESH = pl.DeviceIdType.MESH
F32 = jnp.float32
BF16 = jnp.bfloat16
ORDERS = ((0, 1, 2), (1, 2, 0), (2, 0, 1))
LHS_ROWS = 992
ROW_C, ROW_R, ROW_BIAS, ROW_GAIN = 768, 896, 960, 961
VMEM_LIMIT = 67043328


def place():
    r = lax.axis_index("row")
    m = lax.axis_index("col")
    x = (m // 8) * 2 + r % 2
    y = r // 2
    z = (m // 2) % 4
    c = m % 2
    return x, y, z, c


def device(x, y, z, c):
    return (y * 2 + x % 2, (x // 2) * 8 + z * 2 + c)


def trig_tables():
    quarter = 1536
    freq = 10000.0 ** (-np.arange(quarter, dtype=np.float64) / quarter)
    coarse = 8.0 * np.arange(16, dtype=np.float64)[:, None] * freq[None, :]
    fine = np.arange(8, dtype=np.float64)[:, None] * freq[None, :]
    f = lambda a: a.astype(np.float32)
    return f(np.sin(coarse)), f(np.cos(coarse)), f(np.sin(fine)), f(np.cos(fine))


def prep_kernel(
    pown, p2d, bias_ref, gain_ref, sa, ca, sb, cb, wp_hbm, wq_hbm,
    buf, rsbuf, wout, rpos, cpos,
    wp, lhs, wq, emb, res, mu, rsown,
    ssem, rsem, pss, prs, xss, xrs, lsem, wsem, osem,
):
    x, y, z, c = place()
    coord = (x, y, z)
    row = lax.axis_index("row")
    col = lax.axis_index("col")

    def near(axis, d):
        t = list(coord)
        t[axis] = (t[axis] + d) % 4
        return device(t[0], t[1], t[2], c)

    partner = device(x, y, z, 1 - c)

    def piece(p, ph, val, core, half=None):
        order = ORDERS[p]
        idx = []
        for b in range(3):
            if b in order[:ph]:
                idx.append(pl.ds(0, 4))
            elif b == order[ph]:
                idx.append(val)
            else:
                idx.append(coord[b])
        tail = () if half is None else (half,)
        if half is None:
            return buf.at[(p, *idx, core)]
        return buf.at[(p, *idx, core, half)]

    def ring(p, ph, slot, recv):
        axis = ORDERS[p][ph]
        own = coord[axis]
        if slot < 2:
            if recv:
                src = piece(p, ph, (own + (3 if slot == 0 else 1)) % 4, c)
                dst = src
            else:
                dst = piece(p, ph, own, c)
                src = pown.at[p] if ph == 0 else dst
        else:
            if recv:
                src = piece(p, ph, (own + 2) % 4, c, slot - 2)
            else:
                src = piece(p, ph, (own + (3 if slot == 2 else 1)) % 4, c, slot - 2)
            dst = src
        to = near(axis, 1 if slot % 2 == 0 else 3)
        return pltpu.make_async_remote_copy(
            src_ref=src, dst_ref=dst, send_sem=ssem.at[p, ph, slot], recv_sem=rsem.at[p, ph, slot],
            device_id=to, device_id_type=MESH)

    def across(p, k, recv):
        core = 1 - c if recv else c
        own = coord[ORDERS[p][2]]
        val = (own, (own + 3) % 4, (own + 1) % 4, (own + 2) % 4, (own + 2) % 4)[k]
        ref = piece(p, 2, val, core, None if k < 3 else k - 3)
        return pltpu.make_async_remote_copy(
            src_ref=ref, dst_ref=ref, send_sem=pss.at[p, k], recv_sem=prs.at[p, k],
            device_id=partner, device_id_type=MESH)

    def rs_copy(step, d, recv):
        if step == 0:
            core = 1 - c if recv else c
            dst = rsbuf.at[x, y, z, core]
            src = dst if recv else rsown
            to = partner
        else:
            axis = step - 1
            idx = []
            for b in range(3):
                if b < axis:
                    idx.append(pl.ds(0, 4))
                elif b == axis:
                    idx.append((coord[b] + 4 - d) % 4 if recv else coord[b])
                else:
                    idx.append(coord[b])
            dst = rsbuf.at[tuple(idx)]
            src = dst
            to = near(axis, d)
        return pltpu.make_async_remote_copy(
            src_ref=src, dst_ref=dst, send_sem=xss.at[step, d], recv_sem=xrs.at[step, d],
            device_id=to, device_id_type=MESH)

    def start_phase(ph):
        for slot in (0, 1):
            for p in range(3):
                ring(p, ph, slot, False).start()

    def forward_phase(ph):
        for slot in (0, 1):
            for p in range(3):
                ring(p, ph, slot, True).wait_recv()
                ring(p, ph, slot + 2, False).start()
                if ph == 2:
                    across(p, 1 + slot, False).start()

    def finish_phase(ph):
        for slot in (2, 3):
            for p in range(3):
                ring(p, ph, slot, True).wait_recv()
                if ph == 2:
                    across(p, 1 + slot, False).start()

    def rs_step(step):
        for d in ((0,) if step == 0 else (1, 2, 3)):
            rs_copy(step, d, False).start()

    def rs_wait(step):
        for d in ((0,) if step == 0 else (1, 2, 3)):
            rs_copy(step, d, True).wait_recv()

    wp_copies = [pltpu.make_async_copy(wp_hbm.at[pl.ds(i * 192, 192)], wp.at[pl.ds(i * 192, 192)], lsem.at[i]) for i in range(4)]
    for cp in wp_copies:
        cp.start()
    wq_copies = [pltpu.make_async_copy(wq_hbm.at[b // 3, b % 3], wq.at[b], wsem.at[b]) for b in range(9)]
    for cp in wq_copies:
        cp.start()

    barrier = pltpu.get_barrier_semaphore()
    peers = [near(a, d) for a in range(3) for d in (1, 2, 3)] + [partner]
    for peer in peers:
        pl.semaphore_signal(barrier, inc=1, device_id=peer, device_id_type=MESH)
    pl.semaphore_wait(barrier, len(peers))

    start_phase(0)
    own_copy = pltpu.make_async_copy(pown, buf.at[pl.ds(0, 3), x, y, z, c], osem.at[0])
    own_copy.start()

    gain = gain_ref[...]
    gain_lo, gain_hi = gain[:, :3072], gain[:, 3072:]
    bias = bias_ref[...]

    lhs[ROW_C:ROW_C + 128, 0:3072] = jnp.zeros((128, 3072), BF16)
    lhs[ROW_R:ROW_R + 64, 3072:6144] = jnp.zeros((64, 3072), BF16)
    sbv, cbv = sb[...], cb[...]
    for t in range(8):
        sins, coss = [], []
        for u in (2 * t, 2 * t + 1):
            sav, cav = sa[u:u + 1, :], ca[u:u + 1, :]
            sins.append(sav * cbv + cav * sbv)
            coss.append(cav * cbv - sav * sbv)
        table = jnp.concatenate([jnp.concatenate(sins, 0), jnp.concatenate(coss, 0)], axis=1)
        mu[16 * t:16 * t + 16, :] = jnp.broadcast_to(jnp.sum(table, axis=1, keepdims=True) * (1.0 / 6144), (16, 128))
        lhs[ROW_C + 16 * t:ROW_C + 16 * t + 16, 3072:6144] = (table * gain_hi).astype(BF16)
        if t < 4:
            lhs[ROW_R + 16 * t:ROW_R + 16 * t + 16, 0:3072] = (table * gain_lo).astype(BF16)
    bias_c = (bias - jnp.mean(bias, axis=1, keepdims=True)) * gain
    tail_rows = lax.broadcasted_iota(jnp.int32, (32, 6144), 0)
    lhs[ROW_BIAS:ROW_BIAS + 32, :] = jnp.where(
        tail_rows == 0, bias_c, jnp.where(tail_rows == 1, gain, 0.0)).astype(BF16)

    for cp in wp_copies:
        cp.wait()
    forward_phase(0)

    def own_table(n):
        sav, cav = sa[pl.ds(n, 1), :], ca[pl.ds(n, 1), :]
        return jnp.concatenate([sav * cbv + cav * sbv, cav * cbv - sav * sbv], axis=1)

    t_row, t_col = own_table(row), own_table(col)
    pixels = p2d[...]
    total = jnp.zeros((64, 1), F32)
    for n in range(12):
        lo = n * 512
        e = jnp.dot(pixels, wp[:, lo:lo + 512], preferred_element_type=F32) + bias[:, lo:lo + 512]
        e = e.reshape(8, 8, 512)
        if n < 6:
            e = e + t_row[:, lo:lo + 512].reshape(8, 1, 512)
        else:
            e = e + t_col[:, lo - 3072:lo - 2560].reshape(1, 8, 512)
        e = e.reshape(64, 512)
        emb[:, lo:lo + 512] = e
        total = total + jnp.sum(e, axis=1, keepdims=True)
    mean = total * (1.0 / 6144)
    square = jnp.zeros((64, 1), F32)
    for n in range(12):
        d = emb[:, n * 512:n * 512 + 512] - mean
        square = square + jnp.sum(d * d, axis=1, keepdims=True)
    rstd = lax.rsqrt(square * (1.0 / 6144) + NORM_EPS)
    rs_wide = jnp.concatenate([jnp.broadcast_to(rstd, (64, 128)), jnp.zeros((64, 128), F32)], axis=0)
    rsown[...] = rs_wide.T[0:1, :]

    finish_phase(0)
    own_copy.wait()
    start_phase(1)
    rs_own_copy = pltpu.make_async_copy(rsown, rsbuf.at[x, y, z, c], osem.at[1])
    rs_own_copy.start()
    rs_step(0)

    def center(i, carry):
        w = wp[pl.ds(pl.multiple_of(i * 48, 48), 48), :].astype(F32)
        w = (w - jnp.mean(w, axis=1, keepdims=True)) * gain
        lhs[pl.ds(pl.multiple_of(i * 48, 48), 48), :] = w.astype(BF16)
        return carry

    lax.fori_loop(0, 8, center, 0)
    forward_phase(1)
    rs_own_copy.wait()
    rs_wait(0)
    rs_step(1)
    lax.fori_loop(8, 16, center, 0)
    finish_phase(1)
    start_phase(2)
    for p in range(3):
        across(p, 0, False).start()
    rs_wait(1)
    rs_step(2)
    for cp in wq_copies:
        cp.wait()

    def product(it, carry):
        pair = it // 2
        mt = it % 2
        rows = pl.ds(pl.multiple_of(mt * 496, 496), 496)
        second = jnp.minimum(2 * pair + 1, 8)
        w = jnp.concatenate([wq[2 * pair], wq[second]], axis=1)
        res[pair, rows, :] = jnp.dot(lhs[rows, :], w, preferred_element_type=F32)

        @pl.when(it == 2)
        def _():
            rs_wait(2)
            rs_step(3)

        @pl.when(it == 8)
        def _():
            forward_phase(2)
        return carry

    lax.fori_loop(0, 10, product, 0)

    mus = mu[...]
    for b in range(9):
        lanes = slice((b % 2) * 128, (b % 2) * 128 + 128)
        w = res[b // 2, 0:768, lanes]
        gsum = res[b // 2, ROW_GAIN:ROW_GAIN + 1, lanes]
        rp = res[b // 2, ROW_R:ROW_R + 64, lanes] - mus[:64] * gsum + res[b // 2, ROW_BIAS:ROW_BIAS + 1, lanes]
        cp = res[b // 2, ROW_C:ROW_C + 128, lanes] - mus * gsum
        if b < 6:
            w = w - jnp.mean(w, axis=1, keepdims=True)
            rp = rp - jnp.mean(rp, axis=1, keepdims=True)
            cp = cp - jnp.mean(cp, axis=1, keepdims=True)
        out = slice(b * 128, b * 128 + 128)
        wout[:, out] = w.astype(BF16)
        rpos[:, out] = rp
        cpos[:, out] = cp

    finish_phase(2)
    rs_wait(3)
    for p in range(3):
        for k in range(5):
            across(p, k, True).wait_recv()
    for p in range(3):
        for ph in range(3):
            for slot in range(4):
                ring(p, ph, slot, False).wait_send()
        for k in range(5):
            across(p, k, False).wait_send()
    for step in range(4):
        for d in ((0,) if step == 0 else (1, 2, 3)):
            rs_copy(step, d, False).wait_send()


def prep(pown, p2d, bias, gain, w_patch, w_qkv):
    tables = [jnp.asarray(t) for t in trig_tables()]
    vm = pl.BlockSpec(memory_space=pltpu.VMEM)
    anym = pl.BlockSpec(memory_space=pl.ANY)
    dma = pltpu.SemaphoreType.DMA
    return pl.pallas_call(
        prep_kernel,
        out_shape=(
            jax.ShapeDtypeStruct((3, 4, 4, 4, 2, 2, 32, 256), BF16),
            jax.ShapeDtypeStruct((4, 4, 4, 2, 1, 128), F32),
            jax.ShapeDtypeStruct((768, 1152), BF16),
            jax.ShapeDtypeStruct((64, 1152), F32),
            jax.ShapeDtypeStruct((128, 1152), F32),
        ),
        in_specs=[vm] * 8 + [anym] * 2,
        out_specs=(anym, vm, vm, vm, vm),
        scratch_shapes=[
            pltpu.VMEM((768, 6144), BF16),
            pltpu.VMEM((LHS_ROWS, 6144), BF16),
            pltpu.VMEM((9, 6144, 128), BF16),
            pltpu.VMEM((64, 6144), F32),
            pltpu.VMEM((5, LHS_ROWS, 256), F32),
            pltpu.VMEM((128, 128), F32),
            pltpu.VMEM((1, 128), F32),
            dma((3, 3, 4)), dma((3, 3, 4)), dma((3, 5)), dma((3, 5)),
            dma((4, 4)), dma((4, 4)), dma((4,)), dma((9,)), dma((2,)),
        ],
        compiler_params=pltpu.CompilerParams(collective_id=0, has_side_effects=True, vmem_limit_bytes=VMEM_LIMIT),
        name="prep",
    )(pown, p2d, bias, gain, *tables, w_patch, w_qkv)


def attend_kernel(
    buf, rs_ref, w_ref, rpos, cpos, qk_gain, wo_hbm,
    ctx, wslab,
    tiles, kall, vall, qall, acc, peak,
    tsem, ssem, rsem,
):
    x, y, z, c = place()
    row = lax.axis_index("row")
    x_hi = x // 2

    barrier = pltpu.get_barrier_semaphore()
    slab_to = [device(x_hi * 2 + t % 2, t // 2, row // 2, row % 2) for t in range(8)]
    slab_from = [device(x_hi * 2 + c, z, t // 2, t % 2) for t in range(8)]
    me_target = (row // 2 == z) & (row % 2 == c)
    slot_here = z * 2 + c

    for t in range(8):
        is_self = me_target & (row == t)

        @pl.when(jnp.logical_not(is_self))
        def _():
            pl.semaphore_signal(barrier, inc=1, device_id=slab_to[t], device_id_type=MESH)
        from_self = me_target & (slot_here == t)

        @pl.when(jnp.logical_not(from_self))
        def _():
            pl.semaphore_signal(barrier, inc=1, device_id=slab_from[t], device_id_type=MESH)
    pl.semaphore_wait(barrier, jnp.where(me_target, 14, 16))

    def slab_copy(t):
        return pltpu.make_async_remote_copy(
            src_ref=wo_hbm, dst_ref=wslab.at[slot_here], send_sem=ssem.at[t], recv_sem=rsem.at[slot_here],
            device_id=slab_to[t], device_id_type=MESH)

    def slab_arrival(t):
        return pltpu.make_async_remote_copy(
            src_ref=wo_hbm, dst_ref=wslab.at[t], send_sem=ssem.at[t], recv_sem=rsem.at[t],
            device_id=slab_from[t], device_id_type=MESH)

    def slab_local():
        return pltpu.make_async_copy(wo_hbm, wslab.at[slot_here], rsem.at[slot_here])

    for t in range(8):
        is_self = me_target & (row == t)

        @pl.when(is_self)
        def _():
            slab_local().start()

        @pl.when(jnp.logical_not(is_self))
        def _():
            slab_copy(t).start()

    def tile_copies(n, slot):
        cx, cy, ch = n // 8, (n // 2) % 4, n % 2
        return [
            pltpu.make_async_copy(buf.at[p, cx, cy, pl.ds(ch * 2, 2)], tiles.at[slot, p], tsem.at[slot, p])
            for p in range(3)
        ]

    scale = math.log2(math.e) / math.sqrt(128.0)

    def project(n, slot, first, width):
        cx, cy, ch = n // 8, (n // 2) % 4, n % 2
        p = jnp.concatenate([tiles[slot, q].reshape(256, 256) for q in range(3)], axis=1)
        yv = jnp.dot(p, w_ref[:, first:first + width], preferred_element_type=F32).reshape(4, 8, 8, width)
        r = cy * 2 + cx % 2
        base = (cx // 2) * 64 + ch * 32
        rp = rpos[pl.ds(pl.multiple_of(r * 8, 8), 8), first:first + width]
        cp = cpos[pl.ds(pl.multiple_of(base, 32), 32), first:first + width]
        yv = yv + rp.reshape(1, 8, 1, width) + cp.reshape(4, 1, 8, width)
        rs8 = rs_ref[cx, cy].reshape(8, 128)
        rst = jnp.concatenate([rs8] + [jnp.zeros((120, 128), F32)], axis=0).T
        rst = jnp.where(ch == 0, rst[0:64, 0:4], rst[0:64, 4:8])
        rcol = jnp.concatenate([rst[:, q:q + 1] for q in range(4)], axis=0)
        return yv.reshape(256, width), rcol

    def normed(yh, rcol, gain):
        var = jnp.mean(yh * yh, axis=1, keepdims=True)
        return yh * (rcol * lax.rsqrt(rcol * rcol * var + NORM_EPS)) * gain

    order_count = 32
    for cp in tile_copies(0, 0):
        cp.start()

    def fill(n, carry):
        slot = n % 2

        @pl.when(n + 1 < order_count)
        def _():
            for cp in tile_copies(n + 1, 1 - slot):
                cp.start()
        for cp in tile_copies(n, slot):
            cp.wait()
        cx, cy, ch = n // 8, (n // 2) % 4, n % 2
        yv, rcol = project(n, slot, 384, 768)
        at = pl.ds(pl.multiple_of(n * 256, 256), 256)
        for h in range(3):
            kall[h, at, :] = normed(yv[:, h * 128:h * 128 + 128], rcol, qk_gain[1, h:h + 1, :]).astype(BF16)
            vall[h, at, :] = (yv[:, 384 + h * 128:512 + h * 128] * rcol).astype(BF16)

        @pl.when((cy == y) & (cx % 2 == x % 2))
        def _():
            yq, rq = project(n, slot, 0, 384)
            for h in range(3):
                qh = normed(yq[:, h * 128:h * 128 + 128], rq, qk_gain[0, h:h + 1, :] * scale)
                qh = qh.reshape(4, 8, 8, 128)
                for i in range(8):
                    dst = i * 128 + (cx // 2) * 64 + ch * 32
                    qall[h, pl.ds(pl.multiple_of(dst, 32), 32), :] = qh[:, i].reshape(32, 128).astype(BF16)
        return carry

    lax.fori_loop(0, order_count, fill, 0)

    QT, BK, NCH = 256, 1024, 4
    ones = jnp.ones((BK, 128), BF16)

    def head(h, carry):
        for t in range(NCH):
            acc[t] = jnp.zeros((QT, 256), F32)
            peak[t] = jnp.full((QT, 128), -1e30, F32)

        def block(j, carry2):
            at = pl.ds(pl.multiple_of(j * BK, BK), BK)
            k = kall[h, at, :]
            va = jnp.concatenate([vall[h, at, :], ones], axis=1)
            scores = [
                lax.dot_general(qall[h, t * QT:t * QT + QT, :], k, (((1,), (1,)), ((), ())), preferred_element_type=F32)
                for t in range(NCH)
            ]
            for t in range(NCH):
                old = peak[t][:, :1]
                new = jnp.maximum(old, jnp.max(scores[t], axis=1, keepdims=True))
                p = jnp.exp2(scores[t] - new).astype(BF16)
                acc[t] = acc[t] * jnp.exp2(old - new) + jnp.dot(p, va, preferred_element_type=F32)
                peak[t] = jnp.broadcast_to(new, (QT, 128))
            return carry2

        lax.fori_loop(0, 8192 // BK, block, 0)
        for t in range(NCH):
            a = acc[t]
            ctx[h, t * QT:t * QT + QT, :] = (a[:, :128] / a[:, 128:]).astype(BF16)
        return carry

    lax.fori_loop(0, 3, head, 0)

    for t in range(8):
        from_self = me_target & (slot_here == t)

        @pl.when(from_self)
        def _():
            slab_local().wait()

        @pl.when(jnp.logical_not(from_self))
        def _():
            slab_arrival(t).wait_recv()
        is_self = me_target & (row == t)

        @pl.when(jnp.logical_not(is_self))
        def _():
            slab_copy(t).wait_send()


def attend(buf, rs, w, rpos, cpos, qk_gain, wo):
    vm = pl.BlockSpec(memory_space=pltpu.VMEM)
    anym = pl.BlockSpec(memory_space=pl.ANY)
    dma = pltpu.SemaphoreType.DMA
    return pl.pallas_call(
        attend_kernel,
        out_shape=(
            jax.ShapeDtypeStruct((3, 1024, 128), BF16),
            jax.ShapeDtypeStruct((8, 384, 768), BF16),
        ),
        in_specs=[anym] + [vm] * 5 + [anym],
        out_specs=(vm, anym),
        scratch_shapes=[
            pltpu.VMEM((2, 3, 2, 2, 2, 32, 256), BF16),
            pltpu.VMEM((3, 8192, 128), BF16),
            pltpu.VMEM((3, 8192, 128), BF16),
            pltpu.VMEM((3, 1024, 128), BF16),
            pltpu.VMEM((4, 256, 256), F32),
            pltpu.VMEM((4, 256, 128), F32),
            dma((2, 3)), dma((8,)), dma((8,)),
        ],
        compiler_params=pltpu.CompilerParams(collective_id=1, has_side_effects=True, vmem_limit_bytes=VMEM_LIMIT),
        name="attend",
    )(buf, rs, w, rpos, cpos, qk_gain, wo)


def finish_kernel(ctx, wslab_hbm, out, cbuf, wv, part, rbuf, ssem, rsem, pss, prs, fss, frs, lsem, osem):
    x, y, z, c = place()
    x_hi = x // 2
    row = lax.axis_index("row")
    partner = device(x, y, z, 1 - c)
    wcopy = pltpu.make_async_copy(wslab_hbm, wv, lsem.at[0])
    wcopy.start()

    def core_at(dz):
        return device(x, y, (z + dz) % 4, c)

    def owner(t):
        return (row, t)

    col = lax.axis_index("col")
    barrier = pltpu.get_barrier_semaphore()
    for t in range(16):
        @pl.when(col != t)
        def _():
            pl.semaphore_signal(barrier, inc=1, device_id=owner(t), device_id_type=MESH)
    pl.semaphore_wait(barrier, 15)

    own_copy = pltpu.make_async_copy(ctx, cbuf.at[z, c], osem.at[0])
    own_copy.start()

    def ring(slot, recv):
        if slot < 2:
            if recv:
                src = cbuf.at[(z + (3 if slot == 0 else 1)) % 4, c]
                dst = src
            else:
                src, dst = ctx, cbuf.at[z, c]
        else:
            off = 2 if recv else (3 if slot == 2 else 1)
            src = cbuf.at[(z + off) % 4, c, pl.ds(0, 3), pl.ds((slot - 2) * 512, 512)]
            dst = src
        return pltpu.make_async_remote_copy(
            src_ref=src, dst_ref=dst, send_sem=ssem.at[slot], recv_sem=rsem.at[slot],
            device_id=core_at(1 if slot % 2 == 0 else 3), device_id_type=MESH)

    def across(k, recv):
        core = 1 - c if recv else c
        if k < 3:
            ref = cbuf.at[(z + (0, 3, 1)[k]) % 4, core]
        else:
            ref = cbuf.at[(z + 2) % 4, core, pl.ds(0, 3), pl.ds((k - 3) * 512, 512)]
        src = ctx if (k == 0 and not recv) else ref
        return pltpu.make_async_remote_copy(
            src_ref=src, dst_ref=ref, send_sem=pss.at[k], recv_sem=prs.at[k],
            device_id=partner, device_id_type=MESH)

    ring(0, False).start()
    ring(1, False).start()
    across(0, False).start()
    for slot in (0, 1):
        ring(slot, True).wait_recv()
        ring(slot + 2, False).start()
        across(1 + slot, False).start()
    for slot in (2, 3):
        ring(slot, True).wait_recv()
        across(1 + slot, False).start()
    own_copy.wait()
    wcopy.wait()
    for k in range(5):
        across(k, True).wait_recv()

    slab = z * 2 + c

    def send(t):
        return pltpu.make_async_remote_copy(
            src_ref=part.at[t], dst_ref=rbuf.at[x_hi, slab], send_sem=fss.at[t], recv_sem=frs.at[x_hi, slab],
            device_id=owner(t), device_id_type=MESH)

    def keep(t):
        return pltpu.make_async_copy(part.at[t], rbuf.at[x_hi, slab], osem.at[1])

    def arrival(hi, t):
        return pltpu.make_async_remote_copy(
            src_ref=part.at[0], dst_ref=rbuf.at[hi, t], send_sem=fss.at[t], recv_sem=frs.at[hi, t],
            device_id=owner(t), device_id_type=MESH)

    def tile(i, carry):
        rows = pl.ds(pl.multiple_of(i * 256, 256), 256)
        a = jnp.concatenate([cbuf[t // 2, t % 2, h, rows, :] for t in range(8) for h in range(3)], axis=1)
        s = jnp.dot(a, wv[...].reshape(3072, 768), preferred_element_type=F32).astype(BF16)
        for q in range(4):
            t = i * 4 + q
            part[t] = s[q * 64:q * 64 + 64, :]

            @pl.when(t == col)
            def _():
                rbuf[x_hi, slab] = s[q * 64:q * 64 + 64, :]

            @pl.when(t != col)
            def _():
                send(t).start()
        return carry

    lax.fori_loop(0, 4, tile, 0)
    for t in range(8):
        for hi in range(2):
            @pl.when(hi * 8 + t != col)
            def _():
                arrival(hi, t).wait_recv()
        out[:, t * 768:t * 768 + 768] = (rbuf[0, t].astype(F32) + rbuf[1, t].astype(F32)).astype(BF16)
    for slot in range(4):
        ring(slot, False).wait_send()
    for k in range(5):
        across(k, False).wait_send()
    for t in range(16):
        @pl.when(t != col)
        def _():
            send(t).wait_send()


def finish(ctx, wslab):
    vm = pl.BlockSpec(memory_space=pltpu.VMEM)
    anym = pl.BlockSpec(memory_space=pl.ANY)
    dma = pltpu.SemaphoreType.DMA
    return pl.pallas_call(
        finish_kernel,
        out_shape=jax.ShapeDtypeStruct((64, 6144), BF16),
        in_specs=[anym, anym],
        out_specs=vm,
        scratch_shapes=[
            pltpu.VMEM((4, 2, 3, 1024, 128), BF16),
            pltpu.VMEM((8, 384, 768), BF16),
            pltpu.VMEM((16, 64, 768), BF16),
            pltpu.VMEM((2, 8, 64, 768), BF16),
            dma((4,)), dma((4,)), dma((5,)), dma((5,)), dma((16,)), dma((2, 8)), dma((1,)), dma((2,)),
        ],
        compiler_params=pltpu.CompilerParams(collective_id=2, has_side_effects=True, vmem_limit_bytes=VMEM_LIMIT),
        name="finish",
    )(ctx, wslab)


def local(patches, w_patch, patch_bias, ln_gain, w_qkv, qk_gain, w_out):
    p2d = patches.reshape(64, 768)
    pown = p2d.reshape(2, 32, 3, 256).transpose(2, 0, 1, 3)
    bias = patch_bias.astype(F32)[None, :]
    gain = ln_gain.astype(F32)[None, :]
    buf, rs, w, rpos, cpos = prep(pown, p2d, bias, gain, w_patch, w_qkv.transpose(1, 2, 0, 3))
    ctx, wslab = attend(buf, rs, w, rpos, cpos, qk_gain, w_out.reshape(384, 768))
    return finish(ctx, wslab)


def solution(mesh):
    return jax.shard_map(
        local,
        mesh=mesh,
        in_specs=(
            P("row", "col", None), P(), P(), P(),
            P(None, None, "col", None), P(None, "col", None), P("col", None, "row"),
        ),
        out_specs=P(("row", "col"), None),
        check_vma=False,
    )
```

```python
import math

import numpy as np
import jax
import jax.numpy as jnp
from jax import lax
from jax.experimental import pallas as pl
from jax.experimental.pallas import tpu as pltpu
from jax.sharding import PartitionSpec as P

NORM_EPS = 1e-06
MESH = pl.DeviceIdType.MESH
F32 = jnp.float32
BF16 = jnp.bfloat16
ORDERS = ((0, 1, 2), (1, 2, 0), (2, 0, 1))
LHS_ROWS = 992
ROW_C, ROW_R, ROW_BIAS, ROW_GAIN = 768, 896, 960, 961
VMEM_LIMIT = 67043328
QT, CHAINS = 256, 2


def device(x, y, z, c):
    return (y * 2 + x % 2, (x // 2) * 8 + z * 2 + c)


def trig_tables():
    quarter = 1536
    freq = 10000.0 ** (-np.arange(quarter, dtype=np.float64) / quarter)
    coarse = 8.0 * np.arange(16, dtype=np.float64)[:, None] * freq[None, :]
    fine = np.arange(8, dtype=np.float64)[:, None] * freq[None, :]
    f = lambda a: a.astype(np.float32)
    return f(np.sin(coarse)), f(np.cos(coarse)), f(np.sin(fine)), f(np.cos(fine))


def fused_kernel(
    bg, qk_gain, sa, ca, sb, cb, p_hbm, wp_hbm, wq_hbm, wo_hbm,
    out, buf,
    p2d, rsbuf, rsown, wres, rpos, cpos, cbuf, wslab, part, rbuf,
    ssem, rsem, pss, prs, xss, xrs, lsem, wsem, osem,
    w1s, w1r, wxs, wxr, wrs, wrr,
    css, crs, dss, drs, fss, frs, tsem,
):
    row = lax.axis_index("row")
    col = lax.axis_index("col")
    x = (col // 8) * 2 + row % 2
    y = row // 2
    z = (col // 2) % 4
    c = col % 2
    x_hi, x_lo = x // 2, x % 2
    coord = (x, y, z)

    def near(axis, d):
        t = list(coord)
        t[axis] = (t[axis] + d) % 4
        return device(t[0], t[1], t[2], c)

    partner = device(x, y, z, 1 - c)

    def remote(src, dst, send, recv, to):
        return pltpu.make_async_remote_copy(
            src_ref=src, dst_ref=dst, send_sem=send, recv_sem=recv, device_id=to, device_id_type=MESH)

    def piece(p, ph, val, core, half=None):
        order = ORDERS[p]
        idx = []
        for b in range(3):
            if b in order[:ph]:
                idx.append(pl.ds(0, 4))
            elif b == order[ph]:
                idx.append(val)
            else:
                idx.append(coord[b])
        tail = () if half is None else (pl.ds(half * 32, 32),)
        return buf.at[(p, *idx, core, *tail)]

    SLOTS = ((0, 1), (1, 3), (1, 1), (0, 3), (0, 1), (1, 3))

    def ring(p, ph, slot, recv):
        axis = ORDERS[p][ph]
        own = coord[axis]
        half, d = SLOTS[slot]
        if slot < 4:
            if recv:
                src = dst = piece(p, ph, (own + 4 - d) % 4, c, half)
            else:
                dst = piece(p, ph, own, c, half)
                src = p_hbm.at[pl.ds(half * 32, 32), pl.ds(p * 256, 256)] if ph == 0 else dst
        else:
            src = dst = piece(p, ph, (own + (2 if recv else 4 - d)) % 4, c, half)
        return remote(src, dst, ssem.at[p, ph, slot], rsem.at[p, ph, slot], near(axis, d))

    def across(p, k, recv):
        core = 1 - c if recv else c
        own = coord[ORDERS[p][2]]
        val = (own, (own + 3) % 4, (own + 1) % 4, (own + 2) % 4, (own + 2) % 4)[k]
        ref = piece(p, 2, val, core, None if k < 3 else k - 3)
        return remote(ref, ref, pss.at[p, k], prs.at[p, k], partner)

    def start_phase(ph):
        for slot in range(4):
            for p in range(3):
                ring(p, ph, slot, False).start()

    def forward_phase(ph):
        for slot in (0, 1):
            for p in range(3):
                ring(p, ph, slot, True).wait_recv()
                ring(p, ph, slot + 4, False).start()

    def direct_phase(ph):
        for slot in (2, 3):
            for p in range(3):
                ring(p, ph, slot, True).wait_recv()
                if ph == 2:
                    across(p, slot - 1, False).start()

    def finish_phase(ph):
        for slot in (4, 5):
            for p in range(3):
                ring(p, ph, slot, True).wait_recv()
                if ph == 2:
                    across(p, slot - 1, False).start()

    def rs_copy(step, d, recv):
        if step == 0:
            core = 1 - c if recv else c
            dst = rsbuf.at[x, y, z, core]
            src = dst if recv else rsown
            to = partner
        else:
            axis = step - 1
            idx = []
            for b in range(3):
                if b < axis:
                    idx.append(pl.ds(0, 4))
                elif b == axis:
                    idx.append((coord[b] + 4 - d) % 4 if recv else coord[b])
                else:
                    idx.append(coord[b])
            src = dst = rsbuf.at[tuple(idx)]
            to = near(axis, d)
        return remote(src, dst, xss.at[step, d], xrs.at[step, d], to)

    def rs_step(step):
        for d in ((0,) if step == 0 else (1, 2, 3)):
            rs_copy(step, d, False).start()

    def rs_wait(step):
        for d in ((0,) if step == 0 else (1, 2, 3)):
            rs_copy(step, d, True).wait_recv()

    stays = (y == z) & (c == x_lo)
    w1_to = device(x_hi * 2 + c, z, y, x_lo)

    def w1(recv):
        dst = wslab.at[row] if recv else wslab.at[z * 2 + c]
        return remote(wo_hbm, dst, w1s, w1r, w1_to)

    def w1_local():
        return pltpu.make_async_copy(wo_hbm, wslab.at[row], w1r)

    x_pair = device(x_hi * 2 + 1 - x_lo, y, z, c)

    def wx(recv):
        ref = wslab.at[y * 2 + 1 - x_lo] if recv else wslab.at[row]
        return remote(ref, ref, wxs, wxr, x_pair)

    def wring(which, slot, recv):
        lo = x_lo if which == 0 else 1 - x_lo
        half, d = SLOTS[slot]
        if slot < 4:
            ref = wslab.at[((y + (4 - d if recv else 0)) % 4) * 2 + lo, half]
        else:
            ref = wslab.at[((y + (2 if recv else 4 - d)) % 4) * 2 + lo, half]
        return remote(ref, ref, wrs.at[which, slot], wrr.at[which, slot], near(1, d))

    def wring_start(which):
        for slot in range(4):
            wring(which, slot, False).start()

    def wring_forward(which):
        for slot in (0, 1):
            wring(which, slot, True).wait_recv()
            wring(which, slot + 4, False).start()

    def wring_finish(which):
        for slot in range(2, 6):
            wring(which, slot, True).wait_recv()

    def cring(u, slot, recv):
        h, half = u % 3, u // 3
        d = 1 if slot % 2 == 0 else 3
        if slot < 2:
            ref = cbuf.at[half, h, (z + (4 - d if recv else 0)) % 4, c]
        else:
            ref = cbuf.at[half, h, (z + (2 if recv else 4 - d)) % 4, c, pl.ds((slot - 2) * 256, 256)]
        return remote(ref, ref, css.at[u, slot], crs.at[u, slot], near(2, d))

    def cacross(u, k, recv):
        h, half = u % 3, u // 3
        core = 1 - c if recv else c
        if k < 3:
            ref = cbuf.at[half, h, (z + (0, 3, 1)[k]) % 4, core]
        else:
            ref = cbuf.at[half, h, (z + 2) % 4, core, pl.ds((k - 3) * 256, 256)]
        return remote(ref, ref, dss.at[u, k], drs.at[u, k], partner)

    def ctx_start(u):
        cring(u, 0, False).start()
        cring(u, 1, False).start()
        cacross(u, 0, False).start()

    def ctx_forward(u):
        for slot in (0, 1):
            cring(u, slot, True).wait_recv()
            cring(u, slot + 2, False).start()
            cacross(u, 1 + slot, False).start()

    def ctx_finish(u):
        for slot in (2, 3):
            cring(u, slot, True).wait_recv()
            cacross(u, 1 + slot, False).start()

    def ctx_ready(u):
        for k in range(5):
            cacross(u, k, True).wait_recv()

    slab = z * 2 + c

    def owner(half, t):
        return (t // 4) * 8 + (t % 4) * 2 + half

    def send(half, t):
        return remote(part.at[half * 8 + t], rbuf.at[x_hi, slab], fss.at[half * 8 + t], frs.at[x_hi, slab],
                      (row, owner(half, t)))

    def arrival(hi, t):
        return remote(part.at[0], rbuf.at[hi, t], fss.at[0], frs.at[hi, t], (row, hi * 8 + t))

    p_copy = pltpu.make_async_copy(p_hbm, p2d, osem.at[2])
    p_copy.start()

    barrier = pltpu.get_barrier_semaphore()
    peers = [near(a, d) for a in range(3) for d in (1, 2, 3)] + [partner]
    for peer in peers:
        pl.semaphore_signal(barrier, inc=1, device_id=peer, device_id_type=MESH)

    @pl.when(jnp.logical_not(stays))
    def _():
        pl.semaphore_signal(barrier, inc=1, device_id=w1_to, device_id_type=MESH)
    for t in range(16):
        @pl.when(col != t)
        def _():
            pl.semaphore_signal(barrier, inc=1, device_id=(row, t), device_id_type=MESH)

    def prepare(lhs, wq, emb, res, mu):
        wp = lhs
        wp_copies = [
            pltpu.make_async_copy(wp_hbm.at[pl.ds(i * 192, 192)], wp.at[pl.ds(i * 192, 192)], lsem.at[i])
            for i in range(4)]
        for cp in wp_copies:
            cp.start()
        wq_copies = [pltpu.make_async_copy(wq_hbm.at[b // 3, b % 3], wq.at[b], wsem.at[b]) for b in range(9)]
        for cp in wq_copies:
            cp.start()

        pl.semaphore_wait(barrier, jnp.where(stays, len(peers) + 15, len(peers) + 16))
        start_phase(0)

        @pl.when(stays)
        def _():
            w1_local().start()

        @pl.when(jnp.logical_not(stays))
        def _():
            w1(False).start()
        p_copy.wait()
        own_copies = [
            pltpu.make_async_copy(p2d.at[:, pl.ds(p * 256, 256)], buf.at[p, x, y, z, c], osem.at[3 + p])
            for p in range(3)]
        for cp in own_copies:
            cp.start()

        gain = bg[1:2, :]
        gain_lo, gain_hi = gain[:, :3072], gain[:, 3072:]
        bias = bg[0:1, :]

        lhs[ROW_C:ROW_C + 128, 0:3072] = jnp.zeros((128, 3072), BF16)
        lhs[ROW_R:ROW_R + 64, 3072:6144] = jnp.zeros((64, 3072), BF16)
        sbv, cbv = sb[...], cb[...]
        for t in range(8):
            sins, coss = [], []
            for u in (2 * t, 2 * t + 1):
                sav, cav = sa[u:u + 1, :], ca[u:u + 1, :]
                sins.append(sav * cbv + cav * sbv)
                coss.append(cav * cbv - sav * sbv)
            table = jnp.concatenate([jnp.concatenate(sins, 0), jnp.concatenate(coss, 0)], axis=1)
            mu[16 * t:16 * t + 16, :] = jnp.broadcast_to(
                jnp.sum(table, axis=1, keepdims=True) * (1.0 / 6144), (16, 128))
            lhs[ROW_C + 16 * t:ROW_C + 16 * t + 16, 3072:6144] = (table * gain_hi).astype(BF16)
            if t < 4:
                lhs[ROW_R + 16 * t:ROW_R + 16 * t + 16, 0:3072] = (table * gain_lo).astype(BF16)
        bias_c = (bias - jnp.mean(bias, axis=1, keepdims=True)) * gain
        tail_rows = lax.broadcasted_iota(jnp.int32, (32, 6144), 0)
        lhs[ROW_BIAS:ROW_BIAS + 32, :] = jnp.where(
            tail_rows == 0, bias_c, jnp.where(tail_rows == 1, gain, 0.0)).astype(BF16)

        for cp in wp_copies:
            cp.wait()
        forward_phase(0)

        def own_table(n):
            sav, cav = sa[pl.ds(n, 1), :], ca[pl.ds(n, 1), :]
            return jnp.concatenate([sav * cbv + cav * sbv, cav * cbv - sav * sbv], axis=1)

        t_row, t_col = own_table(row), own_table(col)
        pixels = p2d[...]
        total = jnp.zeros((64, 1), F32)
        for n in range(12):
            lo = n * 512
            e = jnp.dot(pixels, wp[0:768, lo:lo + 512], preferred_element_type=F32) + bias[:, lo:lo + 512]
            e = e.reshape(8, 8, 512)
            if n < 6:
                e = e + t_row[:, lo:lo + 512].reshape(8, 1, 512)
            else:
                e = e + t_col[:, lo - 3072:lo - 2560].reshape(1, 8, 512)
            e = e.reshape(64, 512)
            emb[:, lo:lo + 512] = e
            total = total + jnp.sum(e, axis=1, keepdims=True)
        for cp in own_copies:
            cp.wait()
        direct_phase(0)
        finish_phase(0)
        start_phase(1)
        mean = total * (1.0 / 6144)
        square = jnp.zeros((64, 1), F32)
        for n in range(12):
            d = emb[:, n * 512:n * 512 + 512] - mean
            square = square + jnp.sum(d * d, axis=1, keepdims=True)
        rstd = lax.rsqrt(square * (1.0 / 6144) + NORM_EPS)
        rs_wide = jnp.concatenate([jnp.broadcast_to(rstd, (64, 128)), jnp.zeros((64, 128), F32)], axis=0)
        rsown[...] = rs_wide.T[0:1, :]
        rs_own_copy = pltpu.make_async_copy(rsown, rsbuf.at[x, y, z, c], osem.at[1])
        rs_own_copy.start()
        rs_step(0)

        def center(i, carry):
            w = wp[pl.ds(pl.multiple_of(i * 48, 48), 48), :].astype(F32)
            w = (w - jnp.mean(w, axis=1, keepdims=True)) * gain
            lhs[pl.ds(pl.multiple_of(i * 48, 48), 48), :] = w.astype(BF16)
            return carry

        lax.fori_loop(0, 8, center, 0)
        forward_phase(1)
        rs_own_copy.wait()
        rs_wait(0)
        rs_step(1)
        lax.fori_loop(8, 16, center, 0)
        direct_phase(1)
        finish_phase(1)
        start_phase(2)
        for p in range(3):
            across(p, 0, False).start()
        rs_wait(1)
        rs_step(2)
        for cp in wq_copies:
            cp.wait()

        def product(it, carry):
            pair = it // 2
            rows = pl.ds(pl.multiple_of((it % 2) * 496, 496), 496)
            second = jnp.minimum(2 * pair + 1, 8)
            w = jnp.concatenate([wq[2 * pair], wq[second]], axis=1)
            res[pair, rows, :] = jnp.dot(lhs[rows, :], w, preferred_element_type=F32)

            @pl.when(it == 2)
            def _():
                rs_wait(2)
                rs_step(3)

            @pl.when(it == 5)
            def _():
                forward_phase(2)

            @pl.when(it == 8)
            def _():
                direct_phase(2)
            return carry

        lax.fori_loop(0, 10, product, 0)

        mus = mu[...]
        for b in range(9):
            lanes = slice((b % 2) * 128, (b % 2) * 128 + 128)
            w = res[b // 2, 0:768, lanes]
            gsum = res[b // 2, ROW_GAIN:ROW_GAIN + 1, lanes]
            rp = res[b // 2, ROW_R:ROW_R + 64, lanes] - mus[:64] * gsum + res[b // 2, ROW_BIAS:ROW_BIAS + 1, lanes]
            cp = res[b // 2, ROW_C:ROW_C + 128, lanes] - mus * gsum
            if b < 6:
                w = w - jnp.mean(w, axis=1, keepdims=True)
                rp = rp - jnp.mean(rp, axis=1, keepdims=True)
                cp = cp - jnp.mean(cp, axis=1, keepdims=True)
            lanes = slice(b * 128, b * 128 + 128)
            wres[:, lanes] = w.astype(BF16)
            rpos[:, lanes] = rp
            cpos[:, lanes] = cp
        finish_phase(2)
        rs_wait(3)

        @pl.when(stays)
        def _():
            w1_local().wait()

        @pl.when(jnp.logical_not(stays))
        def _():
            w1(True).wait_recv()
        wx(False).start()
        wring_start(0)
        for p in range(3):
            for k in range(5):
                across(p, k, True).wait_recv()

    pl.run_scoped(
        prepare,
        pltpu.VMEM((LHS_ROWS, 6144), BF16),
        pltpu.VMEM((9, 6144, 128), BF16),
        pltpu.VMEM((64, 6144), F32),
        pltpu.VMEM((5, LHS_ROWS, 256), F32),
        pltpu.VMEM((128, 128), F32),
    )

    def attend(tiles, kall, vall, qall):
        def tile_copies(n, slot):
            return [
                pltpu.make_async_copy(buf.at[p, n // 4, n % 4], tiles.at[slot, p], tsem.at[slot, p])
                for p in range(3)]

        scale = math.log2(math.e) / math.sqrt(128.0)

        def project(n, slot, first, width):
            cx, cy = n // 4, n % 4
            p = jnp.concatenate([tiles[slot, q].reshape(512, 256) for q in range(3)], axis=1)
            yv = jnp.dot(p, wres[:, first:first + width], preferred_element_type=F32).reshape(8, 8, 8, width)
            r = cy * 2 + cx % 2
            rp = rpos[pl.ds(pl.multiple_of(r * 8, 8), 8), first:first + width]
            cp = cpos[pl.ds(pl.multiple_of((cx // 2) * 64, 64), 64), first:first + width]
            yv = yv + rp.reshape(1, 8, 1, width) + cp.reshape(8, 1, 8, width)
            rst = jnp.concatenate([rsbuf[cx, cy].reshape(8, 128), jnp.zeros((120, 128), F32)], axis=0).T
            rcol = jnp.concatenate([rst[0:64, q:q + 1] for q in range(8)], axis=0)
            return yv.reshape(512, width), rcol

        def normed(yh, rcol, gain):
            var = jnp.mean(yh * yh, axis=1, keepdims=True)
            return yh * (rcol * lax.rsqrt(rcol * rcol * var + NORM_EPS)) * gain

        for cp in tile_copies(0, 0):
            cp.start()

        def fill(n, carry):
            slot = n % 2

            @pl.when(n + 1 < 16)
            def _():
                for cp in tile_copies(n + 1, 1 - slot):
                    cp.start()
            for cp in tile_copies(n, slot):
                cp.wait()
            yv, rcol = project(n, slot, 384, 768)
            at = pl.ds(pl.multiple_of(n * 512, 512), 512)
            for h in range(3):
                kall[h, at, :] = normed(yv[:, h * 128:h * 128 + 128], rcol, qk_gain[h, 1:2, :]).astype(BF16)
                vall[h, at, :] = (yv[:, 384 + h * 128:512 + h * 128] * rcol).astype(BF16)

            @pl.when((n % 4 == y) & ((n // 4) % 2 == x_lo))
            def _():
                yq, rq = project(n, slot, 0, 384)
                for h in range(3):
                    qh = normed(yq[:, h * 128:h * 128 + 128], rq, qk_gain[h, 0:1, :] * scale).reshape(8, 8, 8, 128)
                    for i in range(8):
                        dst = (n // 8) * 512 + i * 64
                        qall[h, pl.ds(pl.multiple_of(dst, 64), 64), :] = qh[:, i].reshape(64, 128).astype(BF16)

            @pl.when(n == 12)
            def _():
                wring_forward(0)
                wx(True).wait_recv()
                wring_start(1)
            return carry

        lax.fori_loop(0, 16, fill, 0)

        ones = jnp.ones((8192, 128), BF16)

        def partial_rows(half, i, heads):
            rows = pl.ds(pl.multiple_of(i * 256, 256), 256)
            total = None
            for h in heads:
                a = jnp.concatenate([cbuf[half, h, t // 2, t % 2, rows, :] for t in range(8)], axis=1)
                w = jnp.concatenate(
                    [wslab[t, h * 128 // 192, (h * 128) % 192:(h * 128) % 192 + 128, :] if h != 1 else
                     jnp.concatenate([wslab[t, 0, 128:192, :], wslab[t, 1, 0:64, :]], axis=0) for t in range(8)], axis=0)
                d = jnp.dot(a, w, preferred_element_type=F32)
                total = d if total is None else total + d
            return total

        def ship(half, i, rows):
            for q in range(4):
                t = i * 4 + q
                part[half * 8 + t] = rows[q * 64:q * 64 + 64, :]

                @pl.when(owner(half, t) == col)
                def _():
                    rbuf[x_hi, slab] = rows[q * 64:q * 64 + 64, :]

                @pl.when(owner(half, t) != col)
                def _():
                    send(half, t).start()

        def unit(u, carry):
            h, half = u % 3, u // 3
            k = kall[h]
            va = jnp.concatenate([vall[h], ones], axis=1)
            scores = [
                lax.dot_general(
                    qall[h, pl.ds(pl.multiple_of(half * 512 + t * QT, QT), QT), :], k,
                    (((1,), (1,)), ((), ())), preferred_element_type=F32)
                for t in range(CHAINS)]
            for t in range(CHAINS):
                p = jnp.exp2(scores[t] - jnp.max(scores[t], axis=1, keepdims=True)).astype(BF16)
                a = jnp.dot(p, va, preferred_element_type=F32)
                cbuf[half, h, z, c, t * QT:t * QT + QT, :] = (a[:, :128] / a[:, 128:]).astype(BF16)

            @pl.when(u >= 2)
            def _():
                ctx_finish(u - 2)

            @pl.when(u >= 1)
            def _():
                ctx_forward(u - 1)
            ctx_start(u)

            @pl.when(u == 1)
            def _():
                wring_forward(1)

            @pl.when(u == 4)
            def _():
                wring_finish(0)
                wring_finish(1)
                for v in range(3):
                    ctx_ready(v)

                def tile(i, carry2):
                    ship(0, i, partial_rows(0, i, (0, 1, 2)).astype(BF16))
                    return carry2
                lax.fori_loop(0, 2, tile, 0)
            return carry

        lax.fori_loop(0, 6, unit, 0)
        ctx_finish(4)
        for v in (3, 4):
            ctx_ready(v)
        ctx_forward(5)
        ctx_finish(5)
        ctx_ready(5)

        def last_tile(i, carry):
            ship(1, i, partial_rows(1, i, (0, 1, 2)).astype(BF16))
            return carry
        lax.fori_loop(0, 2, last_tile, 0)

    pl.run_scoped(
        attend,
        pltpu.VMEM((2, 3, 4, 2, 64, 256), BF16),
        pltpu.VMEM((3, 8192, 128), BF16),
        pltpu.VMEM((3, 8192, 128), BF16),
        pltpu.VMEM((3, 1024, 128), BF16),
    )

    for t in range(8):
        for hi in range(2):
            @pl.when(hi * 8 + t != col)
            def _():
                arrival(hi, t).wait_recv()
        out[:, t * 768:t * 768 + 768] = (rbuf[0, t].astype(F32) + rbuf[1, t].astype(F32)).astype(BF16)

    for p in range(3):
        for ph in range(3):
            for slot in range(6):
                ring(p, ph, slot, False).wait_send()
        for k in range(5):
            across(p, k, False).wait_send()
    for step in range(4):
        for d in ((0,) if step == 0 else (1, 2, 3)):
            rs_copy(step, d, False).wait_send()

    @pl.when(jnp.logical_not(stays))
    def _():
        w1(False).wait_send()
    wx(False).wait_send()
    for which in range(2):
        for slot in range(6):
            wring(which, slot, False).wait_send()

    for u in range(6):
        for slot in range(4):
            cring(u, slot, False).wait_send()
        for k in range(5):
            cacross(u, k, False).wait_send()
    for half in range(2):
        for t in range(8):
            @pl.when(owner(half, t) != col)
            def _():
                send(half, t).wait_send()


def fused(bg, qk_gain, patches, w_patch, w_qkv, w_out):
    tables = [jnp.asarray(t) for t in trig_tables()]
    vm = pl.BlockSpec(memory_space=pltpu.VMEM)
    anym = pl.BlockSpec(memory_space=pl.ANY)
    dma = pltpu.SemaphoreType.DMA
    return pl.pallas_call(
        fused_kernel,
        out_shape=(
            jax.ShapeDtypeStruct((64, 6144), BF16),
            jax.ShapeDtypeStruct((3, 4, 4, 4, 2, 64, 256), BF16),
        ),
        in_specs=[vm] * 6 + [anym] * 4,
        out_specs=(vm, anym),
        scratch_shapes=[
            pltpu.VMEM((64, 768), BF16),
            pltpu.VMEM((4, 4, 4, 2, 1, 128), F32),
            pltpu.VMEM((1, 128), F32),
            pltpu.VMEM((768, 1152), BF16),
            pltpu.VMEM((64, 1152), F32),
            pltpu.VMEM((128, 1152), F32),
            pltpu.VMEM((2, 3, 4, 2, 512, 128), BF16),
            pltpu.VMEM((8, 2, 192, 768), BF16),
            pltpu.VMEM((16, 64, 768), BF16),
            pltpu.VMEM((2, 8, 64, 768), BF16),
            dma((3, 3, 6)), dma((3, 3, 6)), dma((3, 5)), dma((3, 5)),
            dma((4, 4)), dma((4, 4)), dma((4,)), dma((9,)), dma((6,)),
            dma, dma, dma, dma, dma((2, 6)), dma((2, 6)),
            dma((6, 4)), dma((6, 4)), dma((6, 5)), dma((6, 5)), dma((16,)), dma((2, 8)), dma((2, 3)),
        ],
        compiler_params=pltpu.CompilerParams(collective_id=0, has_side_effects=True, vmem_limit_bytes=VMEM_LIMIT),
        name="fused",
    )(bg, qk_gain, *tables, patches, w_patch, w_qkv, w_out)


def local(patches, w_patch, patch_bias, ln_gain, w_qkv, qk_gain, w_out):
    bg = jnp.stack([patch_bias, ln_gain]).astype(F32)
    out, _ = fused(
        bg, qk_gain.transpose(1, 0, 2), patches.reshape(64, 768), w_patch,
        w_qkv.transpose(1, 2, 0, 3), w_out.reshape(2, 192, 768))
    return out


def solution(mesh):
    return jax.shard_map(
        local,
        mesh=mesh,
        in_specs=(
            P("row", "col", None), P(), P(), P(),
            P(None, None, "col", None), P(None, "col", None), P("col", None, "row"),
        ),
        out_specs=P(("row", "col"), None),
        check_vma=False,
    )
```

```python
import math

import numpy as np
import jax
import jax.numpy as jnp
from jax import lax
from jax.experimental import pallas as pl
from jax.experimental.pallas import tpu as pltpu
from jax.sharding import PartitionSpec as P

NORM_EPS = 1e-06
MESH = pl.DeviceIdType.MESH
F32 = jnp.float32
BF16 = jnp.bfloat16
ORDERS = ((0, 1, 2), (1, 2, 0), (2, 0, 1))
LHS_ROWS, LHS_TILE = 1008, 336
ROW_C, ROW_R, ROW_BIAS, ROW_GAIN = 768, 896, 960, 961
VMEM_LIMIT = 67043328
QT = 128


def device(x, y, z, c):
    return (y * 2 + x % 2, (x // 2) * 8 + z * 2 + c)


def trig_tables():
    quarter = 1536
    freq = 10000.0 ** (-np.arange(quarter, dtype=np.float64) / quarter)
    coarse = 8.0 * np.arange(16, dtype=np.float64)[:, None] * freq[None, :]
    fine = np.arange(8, dtype=np.float64)[:, None] * freq[None, :]
    f = lambda a: a.astype(np.float32)
    return f(np.sin(coarse)), f(np.cos(coarse)), f(np.sin(fine)), f(np.cos(fine))


def fused_kernel(
    bg, qk_gain, sa, ca, sb, cb, p_hbm, wp_hbm, wq_hbm, wo_hbm,
    out, buf,
    p2d, rsbuf, rsown, wres, rpos, cpos, cbuf, wslab, part, rbuf,
    ssem, rsem, pss, prs, xss, xrs, lsem, wsem, osem,
    w1s, w1r, wxs, wxr, wrs, wrr,
    css, crs, dss, drs, fss, frs, tsem, uss, urs,
):
    row = lax.axis_index("row")
    col = lax.axis_index("col")
    x = (col // 8) * 2 + row % 2
    y = row // 2
    z = (col // 2) % 4
    c = col % 2
    x_hi, x_lo = x // 2, x % 2
    coord = (x, y, z)

    def near(axis, d):
        t = list(coord)
        t[axis] = (t[axis] + d) % 4
        return device(t[0], t[1], t[2], c)

    partner = device(x, y, z, 1 - c)

    def remote(src, dst, send, recv, to):
        return pltpu.make_async_remote_copy(
            src_ref=src, dst_ref=dst, send_sem=send, recv_sem=recv, device_id=to, device_id_type=MESH)

    def piece(p, ph, val, core, half=None):
        order = ORDERS[p]
        idx = []
        for b in range(3):
            if b in order[:ph]:
                idx.append(pl.ds(0, 4))
            elif b == order[ph]:
                idx.append(val)
            else:
                idx.append(coord[b])
        tail = () if half is None else (pl.ds(half * 32, 32),)
        return buf.at[(p, *idx, core, *tail)]

    SLOTS = ((0, 1), (1, 3), (1, 1), (0, 3), (0, 1), (1, 3))

    def cast(p, ph, d, recv):
        axis = ORDERS[p][ph]
        dst = piece(p, ph, (coord[axis] + (4 - d if recv else 0)) % 4, c)
        src = p_hbm.at[:, pl.ds(p * 256, 256)] if ph == 0 and not recv else dst
        return remote(src, dst, uss.at[p, ph, d], urs.at[p, ph, d], near(axis, d))

    def cast_start(ph):
        for d in (1, 3, 2):
            for p in range(3):
                cast(p, ph, d, False).start()

    def cast_wait(ph):
        for d in (1, 3, 2):
            for p in range(3):
                cast(p, ph, d, True).wait_recv()

    def ring(p, slot, recv):
        axis = ORDERS[p][2]
        own = coord[axis]
        half, d = SLOTS[slot]
        if slot < 4:
            src = dst = piece(p, 2, (own + (4 - d if recv else 0)) % 4, c, half)
        else:
            src = dst = piece(p, 2, (own + (2 if recv else 4 - d)) % 4, c, half)
        return remote(src, dst, ssem.at[p, slot], rsem.at[p, slot], near(axis, d))

    def across(p, k, recv):
        core = 1 - c if recv else c
        own = coord[ORDERS[p][2]]
        val = (own, (own + 3) % 4, (own + 1) % 4, (own + 2) % 4, (own + 2) % 4)[k]
        ref = piece(p, 2, val, core, None if k < 3 else k - 3)
        return remote(ref, ref, pss.at[p, k], prs.at[p, k], partner)

    def start_phase():
        for slot in range(4):
            for p in range(3):
                ring(p, slot, False).start()

    def forward_phase():
        for slot in (0, 1):
            for p in range(3):
                ring(p, slot, True).wait_recv()
                ring(p, slot + 4, False).start()

    def direct_phase():
        for slot in (2, 3):
            for p in range(3):
                ring(p, slot, True).wait_recv()
                across(p, slot - 1, False).start()

    def finish_phase():
        for slot in (4, 5):
            for p in range(3):
                ring(p, slot, True).wait_recv()
                across(p, slot - 1, False).start()

    def across_wait():
        for p in range(3):
            for k in range(5):
                across(p, k, True).wait_recv()

    def rs_copy(step, d, recv):
        if step == 0:
            core = 1 - c if recv else c
            dst = rsbuf.at[x, y, z, core]
            src = dst if recv else rsown
            to = partner
        else:
            axis = step - 1
            idx = []
            for b in range(3):
                if b < axis:
                    idx.append(pl.ds(0, 4))
                elif b == axis:
                    idx.append((coord[b] + 4 - d) % 4 if recv else coord[b])
                else:
                    idx.append(coord[b])
            src = dst = rsbuf.at[tuple(idx)]
            to = near(axis, d)
        return remote(src, dst, xss.at[step, d], xrs.at[step, d], to)

    def rs_step(step):
        for d in ((0,) if step == 0 else (1, 2, 3)):
            rs_copy(step, d, False).start()

    def rs_wait(step):
        for d in ((0,) if step == 0 else (1, 2, 3)):
            rs_copy(step, d, True).wait_recv()

    stays = (y == z) & (c == x_lo)
    w1_to = device(x_hi * 2 + c, z, y, x_lo)

    def w1(recv):
        dst = wslab.at[row] if recv else wslab.at[z * 2 + c]
        return remote(wo_hbm, dst, w1s, w1r, w1_to)

    def w1_local():
        return pltpu.make_async_copy(wo_hbm, wslab.at[row], w1r)

    x_pair = device(x_hi * 2 + 1 - x_lo, y, z, c)

    def wx(recv):
        ref = wslab.at[y * 2 + 1 - x_lo] if recv else wslab.at[row]
        return remote(ref, ref, wxs, wxr, x_pair)

    def wring(which, slot, recv):
        lo = x_lo if which == 0 else 1 - x_lo
        half, d = SLOTS[slot]
        if slot < 4:
            ref = wslab.at[((y + (4 - d if recv else 0)) % 4) * 2 + lo, half]
        else:
            ref = wslab.at[((y + (2 if recv else 4 - d)) % 4) * 2 + lo, half]
        return remote(ref, ref, wrs.at[which, slot], wrr.at[which, slot], near(1, d))

    def w1_wait():
        @pl.when(stays)
        def _():
            w1_local().wait()

        @pl.when(jnp.logical_not(stays))
        def _():
            w1(True).wait_recv()

    def wring_start(which):
        for slot in range(4):
            wring(which, slot, False).start()

    def wring_forward(which):
        for slot in (0, 1):
            wring(which, slot, True).wait_recv()
            wring(which, slot + 4, False).start()

    def wring_finish(which):
        for slot in range(2, 6):
            wring(which, slot, True).wait_recv()

    def cring(v, slot, recv):
        d = 1 if slot % 2 == 0 else 3
        if slot < 2:
            ref = cbuf.at[v, (z + (4 - d if recv else 0)) % 4, c]
        else:
            ref = cbuf.at[v, (z + (2 if recv else 4 - d)) % 4, c, pl.ds(0, 3), pl.ds((slot - 2) * 64, 64)]
        return remote(ref, ref, css.at[v, slot], crs.at[v, slot], near(2, d))

    def cacross(v, k, recv):
        core = 1 - c if recv else c
        if k < 3:
            ref = cbuf.at[v, (z + (0, 3, 1)[k]) % 4, core]
        else:
            ref = cbuf.at[v, (z + 2) % 4, core, pl.ds(0, 3), pl.ds((k - 3) * 64, 64)]
        return remote(ref, ref, dss.at[v, k], drs.at[v, k], partner)

    def ctx_start(v):
        cring(v, 0, False).start()
        cring(v, 1, False).start()
        cacross(v, 0, False).start()

    def ctx_forward(v):
        for slot in (0, 1):
            cring(v, slot, True).wait_recv()
            cring(v, slot + 2, False).start()
            cacross(v, 1 + slot, False).start()

    def ctx_finish(v):
        for slot in (2, 3):
            cring(v, slot, True).wait_recv()
            cacross(v, 1 + slot, False).start()

    def ctx_ready(v):
        for k in range(5):
            cacross(v, k, True).wait_recv()

    slab = z * 2 + c

    def owner(v, q):
        return (q // 4) * 8 + (q % 4) * 2 + v // 4

    def sixteen(v):
        return pl.ds(pl.multiple_of((v % 4) * 16, 16), 16)

    def send(v, q):
        return remote(part.at[v, pl.ds(q * 16, 16)], rbuf.at[x_hi, slab, sixteen(v)],
                      fss.at[v, q], frs.at[x_hi, slab], (row, owner(v, q)))

    def arrival(hi, t):
        return remote(rbuf.at[hi, t], rbuf.at[hi, t], fss.at[0, 0], frs.at[hi, t], (row, hi * 8 + t))

    p_copy = pltpu.make_async_copy(p_hbm, p2d, osem.at[2])
    p_copy.start()

    barrier = pltpu.get_barrier_semaphore()
    peers = [near(a, d) for a in range(3) for d in (1, 2, 3)] + [partner]
    for peer in peers:
        pl.semaphore_signal(barrier, inc=1, device_id=peer, device_id_type=MESH)

    @pl.when(jnp.logical_not(stays))
    def _():
        pl.semaphore_signal(barrier, inc=1, device_id=w1_to, device_id_type=MESH)
    for t in range(16):
        @pl.when(col != t)
        def _():
            pl.semaphore_signal(barrier, inc=1, device_id=(row, t), device_id_type=MESH)

    def prepare(lhs, wq, emb, res, mu):
        wp = lhs
        wp_copies = [
            pltpu.make_async_copy(wp_hbm.at[pl.ds(i * 192, 192)], wp.at[pl.ds(i * 192, 192)], lsem.at[i])
            for i in range(4)]
        for cp in wp_copies:
            cp.start()
        wq_copies = [pltpu.make_async_copy(wq_hbm.at[b // 3, b % 3], wq.at[b], wsem.at[b]) for b in range(9)]
        for cp in wq_copies:
            cp.start()

        pl.semaphore_wait(barrier, jnp.where(stays, len(peers) + 15, len(peers) + 16))
        cast_start(0)
        p_copy.wait()
        own_copies = [
            pltpu.make_async_copy(p2d.at[:, pl.ds(p * 256, 256)], buf.at[p, x, y, z, c], osem.at[3 + p])
            for p in range(3)]
        for cp in own_copies:
            cp.start()

        gain = bg[1:2, :]
        gain_lo, gain_hi = gain[:, :3072], gain[:, 3072:]
        bias = bg[0:1, :]

        lhs[ROW_C:ROW_C + 128, 0:3072] = jnp.zeros((128, 3072), BF16)
        lhs[ROW_R:ROW_R + 64, 3072:6144] = jnp.zeros((64, 3072), BF16)
        sbv, cbv = sb[...], cb[...]
        for t in range(8):
            sins, coss = [], []
            for u in (2 * t, 2 * t + 1):
                sav, cav = sa[u:u + 1, :], ca[u:u + 1, :]
                sins.append(sav * cbv + cav * sbv)
                coss.append(cav * cbv - sav * sbv)
            table = jnp.concatenate([jnp.concatenate(sins, 0), jnp.concatenate(coss, 0)], axis=1)
            mu[16 * t:16 * t + 16, :] = jnp.broadcast_to(
                jnp.sum(table, axis=1, keepdims=True) * (1.0 / 6144), (16, 128))
            lhs[ROW_C + 16 * t:ROW_C + 16 * t + 16, 3072:6144] = (table * gain_hi).astype(BF16)
            if t < 4:
                lhs[ROW_R + 16 * t:ROW_R + 16 * t + 16, 0:3072] = (table * gain_lo).astype(BF16)
        bias_c = (bias - jnp.mean(bias, axis=1, keepdims=True)) * gain
        tail_rows = lax.broadcasted_iota(jnp.int32, (48, 6144), 0)
        lhs[ROW_BIAS:ROW_BIAS + 48, :] = jnp.where(
            tail_rows == 0, bias_c, jnp.where(tail_rows == 1, gain, 0.0)).astype(BF16)

        for cp in wp_copies:
            cp.wait()
        for cp in own_copies:
            cp.wait()
        cast_wait(0)
        cast_start(1)

        def own_table(n):
            sav, cav = sa[pl.ds(n, 1), :], ca[pl.ds(n, 1), :]
            return jnp.concatenate([sav * cbv + cav * sbv, cav * cbv - sav * sbv], axis=1)

        t_row, t_col = own_table(row), own_table(col)
        pixels = p2d[...]
        total = jnp.zeros((64, 1), F32)
        for n in range(12):
            lo = n * 512
            e = jnp.dot(pixels, wp[0:768, lo:lo + 512], preferred_element_type=F32) + bias[:, lo:lo + 512]
            e = e.reshape(8, 8, 512)
            if n < 6:
                e = e + t_row[:, lo:lo + 512].reshape(8, 1, 512)
            else:
                e = e + t_col[:, lo - 3072:lo - 2560].reshape(1, 8, 512)
            e = e.reshape(64, 512)
            emb[:, lo:lo + 512] = e
            total = total + jnp.sum(e, axis=1, keepdims=True)
        mean = total * (1.0 / 6144)
        square = jnp.zeros((64, 1), F32)
        for n in range(12):
            d = emb[:, n * 512:n * 512 + 512] - mean
            square = square + jnp.sum(d * d, axis=1, keepdims=True)
        rstd = lax.rsqrt(square * (1.0 / 6144) + NORM_EPS)
        rs_wide = jnp.concatenate([jnp.broadcast_to(rstd, (64, 128)), jnp.zeros((64, 128), F32)], axis=0)
        rsown[...] = rs_wide.T[0:1, :]
        rs_own_copy = pltpu.make_async_copy(rsown, rsbuf.at[x, y, z, c], osem.at[1])
        rs_own_copy.start()
        rs_step(0)

        def center(i, carry):
            w = wp[pl.ds(pl.multiple_of(i * 48, 48), 48), :].astype(F32)
            w = (w - jnp.mean(w, axis=1, keepdims=True)) * gain
            lhs[pl.ds(pl.multiple_of(i * 48, 48), 48), :] = w.astype(BF16)
            return carry

        lax.fori_loop(0, 5, center, 0)
        rs_own_copy.wait()
        rs_wait(0)
        rs_step(1)
        lax.fori_loop(5, 11, center, 0)
        rs_wait(1)
        rs_step(2)
        cast_wait(1)
        start_phase()
        for p in range(3):
            across(p, 0, False).start()
        lax.fori_loop(11, 16, center, 0)
        for cp in wq_copies:
            cp.wait()

        def product(it, carry):
            pair = it // 3
            rows = pl.ds(pl.multiple_of((it % 3) * LHS_TILE, LHS_TILE), LHS_TILE)
            second = jnp.minimum(2 * pair + 1, 8)
            w = jnp.concatenate([wq[2 * pair], wq[second]], axis=1)
            res[pair, rows, :] = jnp.dot(lhs[rows, :], w, preferred_element_type=F32)

            @pl.when(it == 0)
            def _():
                rs_wait(2)
                rs_step(3)

            @pl.when(it == 5)
            def _():
                forward_phase()

            @pl.when(it == 10)
            def _():
                direct_phase()

            @pl.when(it == 14)
            def _():
                finish_phase()
            return carry

        lax.fori_loop(0, 15, product, 0)

        mus = mu[...]
        for b in range(9):
            lanes = slice((b % 2) * 128, (b % 2) * 128 + 128)
            w = res[b // 2, 0:768, lanes]
            gsum = res[b // 2, ROW_GAIN:ROW_GAIN + 1, lanes]
            rp = res[b // 2, ROW_R:ROW_R + 64, lanes] - mus[:64] * gsum + res[b // 2, ROW_BIAS:ROW_BIAS + 1, lanes]
            cp = res[b // 2, ROW_C:ROW_C + 128, lanes] - mus * gsum
            if b < 6:
                w = w - jnp.mean(w, axis=1, keepdims=True)
                rp = rp - jnp.mean(rp, axis=1, keepdims=True)
                cp = cp - jnp.mean(cp, axis=1, keepdims=True)
            lanes = slice(b * 128, b * 128 + 128)
            wres[:, lanes] = w.astype(BF16)
            rpos[:, lanes] = rp
            cpos[:, lanes] = cp
        rs_wait(3)

        across_wait()

        @pl.when(stays)
        def _():
            w1_local().start()

        @pl.when(jnp.logical_not(stays))
        def _():
            w1(False).start()

    pl.run_scoped(
        prepare,
        pltpu.VMEM((LHS_ROWS, 6144), BF16),
        pltpu.VMEM((9, 6144, 128), BF16),
        pltpu.VMEM((64, 6144), F32),
        pltpu.VMEM((5, LHS_ROWS, 256), F32),
        pltpu.VMEM((128, 128), F32),
    )

    def attend(tiles, feats, feats2, kall, vall, qall):
        def tile_copies(n, slot):
            return [
                pltpu.make_async_copy(buf.at[p, n // 4, n % 4], tiles.at[slot, p], tsem.at[slot, p])
                for p in range(3)]

        def tile_start(n, slot):
            for cp in tile_copies(n, slot):
                cp.start()

        def tile_wait(n, slot):
            for cp in tile_copies(n, slot):
                cp.wait()

        scale = math.log2(math.e) / math.sqrt(128.0)

        def project(n, slot, first, width):
            cx, cy = n // 4, n % 4
            p = jnp.concatenate([tiles[slot, q].reshape(512, 256) for q in range(3)], axis=1)
            yv = jnp.dot(p, wres[:, first:first + width], preferred_element_type=F32).reshape(8, 8, 8, width)
            r = cy * 2 + cx % 2
            rp = rpos[pl.ds(pl.multiple_of(r * 8, 8), 8), first:first + width]
            cp = cpos[pl.ds(pl.multiple_of((cx // 2) * 64, 64), 64), first:first + width]
            yv = yv + rp.reshape(1, 8, 1, width) + cp.reshape(8, 1, 8, width)
            return yv.reshape(512, width)

        def rstd_of(n):
            rows = rsbuf[n // 4, n % 4].reshape(8, 128)
            rst = jnp.concatenate([rows, jnp.zeros((120, 128), F32)], axis=0).T
            return jnp.concatenate([rst[0:64, q:q + 1] for q in range(8)], axis=0)

        def normed(yh, rcol, gain):
            var = jnp.mean(yh * yh, axis=1, keepdims=True)
            return yh * (rcol * lax.rsqrt(rcol * rcol * var + NORM_EPS)) * gain

        def store_kv(n, ref):
            rcol = rstd_of(n)
            at = pl.ds(pl.multiple_of(n * 512, 512), 512)
            for h in range(3):
                yk = ref[:, h * 128:h * 128 + 128]
                kall[h, at, :] = normed(yk, rcol, qk_gain[h, 1:2, :]).astype(BF16)
                vall[h, at, :] = (ref[:, 384 + h * 128:512 + h * 128] * rcol).astype(BF16)

        def store_q(n, slot):
            @pl.when((n % 4 == y) & ((n // 4) % 2 == x_lo))
            def _():
                yq, rq = project(n, slot, 0, 384), rstd_of(n)
                for h in range(3):
                    qh = normed(yq[:, h * 128:h * 128 + 128], rq, qk_gain[h, 0:1, :] * scale).reshape(8, 8, 8, 128)
                    for t in range(4):
                        for i in range(8):
                            dst = (n // 8) * 512 + t * 128 + i * 16
                            qall[h, pl.ds(pl.multiple_of(dst, 16), 16), :] = (
                                qh[2 * t:2 * t + 2, i].reshape(16, 128).astype(BF16))

        tile_start(0, 0)
        tile_start(1, 1)
        tile_wait(0, 0)
        store_q(0, 0)
        feats[...] = project(0, 0, 384, 768)
        tile_start(2, 0)

        def fill(m, carry):
            n = 2 * m
            tile_wait(n + 1, 1)
            store_q(n + 1, 1)
            feats2[...] = project(n + 1, 1, 384, 768)
            store_kv(n, feats)

            @pl.when(m < 7)
            def _():
                tile_start(n + 3, 1)
                tile_wait(n + 2, 0)
                store_q(n + 2, 0)
            nxt = jnp.minimum(n + 2, 14)
            feats[...] = project(nxt, 0, 384, 768)
            store_kv(n + 1, feats2)

            @pl.when(m < 6)
            def _():
                tile_start(n + 4, 0)

            @pl.when(m == 5)
            def _():
                w1_wait()
                wx(False).start()
                wring_start(0)
            return carry

        lax.fori_loop(0, 8, fill, 0)

        ones = jnp.ones((8192, 128), BF16)

        def project_out(v):
            a = jnp.concatenate([cbuf[v, t // 2, t % 2, h] for h in range(3) for t in range(8)], axis=1)
            w = []
            for h in range(3):
                for t in range(8):
                    if h == 0:
                        w.append(wslab[t, 0, 0:128, :])
                    elif h == 2:
                        w.append(wslab[t, 1, 64:192, :])
                    else:
                        w.append(wslab[t, 0, 128:192, :])
                        w.append(wslab[t, 1, 0:64, :])
            rows = jnp.dot(a, jnp.concatenate(w, axis=0), preferred_element_type=F32).astype(BF16)
            part[v] = rows
            for q in range(8):
                @pl.when(owner(v, q) == col)
                def _():
                    rbuf[x_hi, slab, sixteen(v), :] = rows[q * 16:q * 16 + 16, :]

        def ship(v):
            for q in range(8):
                @pl.when(owner(v, q) != col)
                def _():
                    send(v, q).start()

        def unit(v, carry):
            at = pl.ds(pl.multiple_of(v * QT, QT), QT)
            scores = [
                lax.dot_general(qall[h, at, :], kall[h], (((1,), (1,)), ((), ())), preferred_element_type=F32)
                for h in range(3)]
            for h in range(3):
                p = jnp.exp2(scores[h] - jnp.max(scores[h], axis=1, keepdims=True)).astype(BF16)
                a = jnp.dot(p, jnp.concatenate([vall[h], ones], axis=1), preferred_element_type=F32)
                cbuf[v, z, c, h] = (a[:, :128] / a[:, 128:]).astype(BF16)

            @pl.when(v >= 2)
            def _():
                ctx_finish(v - 2)

            @pl.when(v >= 1)
            def _():
                ctx_forward(v - 1)
            ctx_start(v)

            @pl.when(v == 1)
            def _():
                wx(True).wait_recv()
                wring_start(1)
                wring_forward(0)

            @pl.when(v == 5)
            def _():
                wring_forward(1)
            return carry

        lax.fori_loop(0, 8, unit, 0)
        wring_finish(0)
        wring_finish(1)

        def tail_unit(v, carry):
            @pl.when(v == 4)
            def _():
                ctx_forward(7)
                ctx_finish(6)

            @pl.when(v == 6)
            def _():
                ctx_finish(7)
            ctx_ready(v)
            project_out(v)

            @pl.when(v < 3)
            def _():
                ship(v)

            @pl.when(v == 6)
            def _():
                for t in range(3, 7):
                    ship(t)
            return carry

        lax.fori_loop(0, 8, tail_unit, 0)
        ship(7)

    pl.run_scoped(
        attend,
        pltpu.VMEM((2, 3, 4, 2, 64, 256), BF16),
        pltpu.VMEM((512, 768), F32),
        pltpu.VMEM((512, 768), F32),
        pltpu.VMEM((3, 8192, 128), BF16),
        pltpu.VMEM((3, 8192, 128), BF16),
        pltpu.VMEM((3, 1024, 128), BF16),
    )

    for t in range(8):
        for hi in range(2):
            @pl.when(hi * 8 + t != col)
            def _():
                arrival(hi, t).wait_recv()
        out[:, t * 768:t * 768 + 768] = (rbuf[0, t].astype(F32) + rbuf[1, t].astype(F32)).astype(BF16)

    for p in range(3):
        for ph in range(2):
            for d in (1, 2, 3):
                cast(p, ph, d, False).wait_send()
        for slot in range(6):
            ring(p, slot, False).wait_send()
        for k in range(5):
            across(p, k, False).wait_send()
    for step in range(4):
        for d in ((0,) if step == 0 else (1, 2, 3)):
            rs_copy(step, d, False).wait_send()

    @pl.when(jnp.logical_not(stays))
    def _():
        w1(False).wait_send()
    wx(False).wait_send()
    for which in range(2):
        for slot in range(6):
            wring(which, slot, False).wait_send()

    def left(v, carry):
        for slot in range(4):
            cring(v, slot, False).wait_send()
        for k in range(5):
            cacross(v, k, False).wait_send()
        for q in range(8):
            @pl.when(owner(v, q) != col)
            def _():
                send(v, q).wait_send()
        return carry

    lax.fori_loop(0, 8, left, 0)


def fused(bg, qk_gain, patches, w_patch, w_qkv, w_out):
    tables = [jnp.asarray(t) for t in trig_tables()]
    vm = pl.BlockSpec(memory_space=pltpu.VMEM)
    anym = pl.BlockSpec(memory_space=pl.ANY)
    dma = pltpu.SemaphoreType.DMA
    return pl.pallas_call(
        fused_kernel,
        out_shape=(
            jax.ShapeDtypeStruct((64, 6144), BF16),
            jax.ShapeDtypeStruct((3, 4, 4, 4, 2, 64, 256), BF16),
        ),
        in_specs=[vm] * 6 + [anym] * 4,
        out_specs=(vm, anym),
        scratch_shapes=[
            pltpu.VMEM((64, 768), BF16),
            pltpu.VMEM((4, 4, 4, 2, 1, 128), F32),
            pltpu.VMEM((1, 128), F32),
            pltpu.VMEM((768, 1152), BF16),
            pltpu.VMEM((64, 1152), F32),
            pltpu.VMEM((128, 1152), F32),
            pltpu.VMEM((8, 4, 2, 3, 128, 128), BF16),
            pltpu.VMEM((8, 2, 192, 768), BF16),
            pltpu.VMEM((8, 128, 768), BF16),
            pltpu.VMEM((2, 8, 64, 768), BF16),
            dma((3, 6)), dma((3, 6)), dma((3, 5)), dma((3, 5)),
            dma((4, 4)), dma((4, 4)), dma((4,)), dma((9,)), dma((6,)),
            dma, dma, dma, dma, dma((2, 6)), dma((2, 6)),
            dma((8, 4)), dma((8, 4)), dma((8, 5)), dma((8, 5)), dma((8, 8)), dma((2, 8)), dma((2, 3)),
            dma((3, 2, 4)), dma((3, 2, 4)),
        ],
        compiler_params=pltpu.CompilerParams(collective_id=0, has_side_effects=True, vmem_limit_bytes=VMEM_LIMIT),
        name="fused",
    )(bg, qk_gain, *tables, patches, w_patch, w_qkv, w_out)


def local(patches, w_patch, patch_bias, ln_gain, w_qkv, qk_gain, w_out):
    bg = jnp.stack([patch_bias, ln_gain]).astype(F32)
    out, _ = fused(
        bg, qk_gain.transpose(1, 0, 2), patches.reshape(64, 768), w_patch,
        w_qkv.transpose(1, 2, 0, 3), w_out.reshape(2, 192, 768))
    return out


def solution(mesh):
    return jax.shard_map(
        local,
        mesh=mesh,
        in_specs=(
            P("row", "col", None), P(), P(), P(),
            P(None, None, "col", None), P(None, "col", None), P("col", None, "row"),
        ),
        out_specs=P(("row", "col"), None),
        check_vma=False,
    )
```

```python
import math

import numpy as np
import jax
import jax.numpy as jnp
from jax import lax
from jax.experimental import pallas as pl
from jax.experimental.pallas import tpu as pltpu
from jax.sharding import PartitionSpec as P

NORM_EPS = 1e-06
MESH = pl.DeviceIdType.MESH
F32 = jnp.float32
BF16 = jnp.bfloat16
ORDERS = ((0, 1, 2), (1, 2, 0), (2, 0, 1))
LHS_ROWS, LHS_TILE = 1008, 336
ROW_C, ROW_R, ROW_BIAS, ROW_GAIN = 768, 896, 960, 961
VMEM_LIMIT = 67043328
QT = 128


def device(x, y, z, c):
    return (y * 2 + x % 2, (x // 2) * 8 + z * 2 + c)


def trig_tables():
    quarter = 1536
    freq = 10000.0 ** (-np.arange(quarter, dtype=np.float64) / quarter)
    coarse = 8.0 * np.arange(16, dtype=np.float64)[:, None] * freq[None, :]
    fine = np.arange(8, dtype=np.float64)[:, None] * freq[None, :]
    f = lambda a: a.astype(np.float32)
    return f(np.sin(coarse)), f(np.cos(coarse)), f(np.sin(fine)), f(np.cos(fine))


def fused_kernel(
    bg, qk_gain, sa, ca, sb, cb, p_hbm, wp_hbm, wq_hbm, wo_hbm,
    out, buf,
    p2d, rsbuf, rsown, wres, rpos, cpos, cbuf, wslab, part, rbuf,
    ssem, rsem, pss, prs, xss, xrs, lsem, wsem, osem,
    w1s, w1r, wxs, wxr, wrs, wrr,
    css, crs, dss, drs, fss, frs, tsem, uss, urs,
):
    row = lax.axis_index("row")
    col = lax.axis_index("col")
    x = (col // 8) * 2 + row % 2
    y = row // 2
    z = (col // 2) % 4
    c = col % 2
    x_hi, x_lo = x // 2, x % 2
    coord = (x, y, z)

    def near(axis, d):
        t = list(coord)
        t[axis] = (t[axis] + d) % 4
        return device(t[0], t[1], t[2], c)

    partner = device(x, y, z, 1 - c)

    def remote(src, dst, send, recv, to):
        return pltpu.make_async_remote_copy(
            src_ref=src, dst_ref=dst, send_sem=send, recv_sem=recv, device_id=to, device_id_type=MESH)

    def piece(p, ph, val, core, half=None):
        order = ORDERS[p]
        idx = []
        for b in range(3):
            if b in order[:ph]:
                idx.append(pl.ds(0, 4))
            elif b == order[ph]:
                idx.append(val)
            else:
                idx.append(coord[b])
        tail = () if half is None else (pl.ds(half * 32, 32),)
        return buf.at[(p, *idx, core, *tail)]

    SLOTS = ((0, 1), (1, 3), (1, 1), (0, 3), (0, 1), (1, 3))

    def cast(p, ph, d, recv):
        axis = ORDERS[p][ph]
        dst = piece(p, ph, (coord[axis] + (4 - d if recv else 0)) % 4, c)
        src = p_hbm.at[:, pl.ds(p * 256, 256)] if ph == 0 and not recv else dst
        return remote(src, dst, uss.at[p, ph, d], urs.at[p, ph, d], near(axis, d))

    def cast_start(ph):
        for d in (1, 3, 2):
            for p in range(3):
                cast(p, ph, d, False).start()

    def cast_wait(ph):
        for d in (1, 3, 2):
            for p in range(3):
                cast(p, ph, d, True).wait_recv()

    def ring(p, slot, recv):
        axis = ORDERS[p][2]
        own = coord[axis]
        half, d = SLOTS[slot]
        if slot < 4:
            src = dst = piece(p, 2, (own + (4 - d if recv else 0)) % 4, c, half)
        else:
            src = dst = piece(p, 2, (own + (2 if recv else 4 - d)) % 4, c, half)
        return remote(src, dst, ssem.at[p, slot], rsem.at[p, slot], near(axis, d))

    def across(p, k, recv):
        core = 1 - c if recv else c
        own = coord[ORDERS[p][2]]
        val = (own, (own + 3) % 4, (own + 1) % 4, (own + 2) % 4, (own + 2) % 4)[k]
        ref = piece(p, 2, val, core, None if k < 3 else k - 3)
        return remote(ref, ref, pss.at[p, k], prs.at[p, k], partner)

    def start_phase():
        for slot in range(4):
            for p in range(3):
                ring(p, slot, False).start()

    def forward_phase():
        for slot in (0, 1):
            for p in range(3):
                ring(p, slot, True).wait_recv()
                ring(p, slot + 4, False).start()

    def direct_phase():
        for slot in (2, 3):
            for p in range(3):
                ring(p, slot, True).wait_recv()
                across(p, slot - 1, False).start()

    def finish_phase():
        for slot in (4, 5):
            for p in range(3):
                ring(p, slot, True).wait_recv()
                across(p, slot - 1, False).start()

    def across_wait():
        for p in range(3):
            for k in range(5):
                across(p, k, True).wait_recv()

    def rs_copy(step, d, recv):
        if step == 0:
            core = 1 - c if recv else c
            dst = rsbuf.at[x, y, z, core]
            src = dst if recv else rsown
            to = partner
        else:
            axis = step - 1
            idx = []
            for b in range(3):
                if b < axis:
                    idx.append(pl.ds(0, 4))
                elif b == axis:
                    idx.append((coord[b] + 4 - d) % 4 if recv else coord[b])
                else:
                    idx.append(coord[b])
            src = dst = rsbuf.at[tuple(idx)]
            to = near(axis, d)
        return remote(src, dst, xss.at[step, d], xrs.at[step, d], to)

    def rs_step(step):
        for d in ((0,) if step == 0 else (1, 2, 3)):
            rs_copy(step, d, False).start()

    def rs_wait(step):
        for d in ((0,) if step == 0 else (1, 2, 3)):
            rs_copy(step, d, True).wait_recv()

    stays = (y == z) & (c == x_lo)
    w1_to = device(x_hi * 2 + c, z, y, x_lo)

    def w1(recv):
        dst = wslab.at[row] if recv else wslab.at[z * 2 + c]
        return remote(wo_hbm, dst, w1s, w1r, w1_to)

    def w1_local():
        return pltpu.make_async_copy(wo_hbm, wslab.at[row], w1r)

    x_pair = device(x_hi * 2 + 1 - x_lo, y, z, c)

    def wx(recv):
        ref = wslab.at[y * 2 + 1 - x_lo] if recv else wslab.at[row]
        return remote(ref, ref, wxs, wxr, x_pair)

    def wring(which, slot, recv):
        lo = x_lo if which == 0 else 1 - x_lo
        half, d = SLOTS[slot]
        if slot < 4:
            ref = wslab.at[((y + (4 - d if recv else 0)) % 4) * 2 + lo, half]
        else:
            ref = wslab.at[((y + (2 if recv else 4 - d)) % 4) * 2 + lo, half]
        return remote(ref, ref, wrs.at[which, slot], wrr.at[which, slot], near(1, d))

    def w1_wait():
        @pl.when(stays)
        def _():
            w1_local().wait()

        @pl.when(jnp.logical_not(stays))
        def _():
            w1(True).wait_recv()

    def wring_start(which):
        for slot in range(4):
            wring(which, slot, False).start()

    def wring_forward(which):
        for slot in (0, 1):
            wring(which, slot, True).wait_recv()
            wring(which, slot + 4, False).start()

    def wring_finish(which):
        for slot in range(2, 6):
            wring(which, slot, True).wait_recv()

    def cring(v, slot, recv):
        d = 1 if slot % 2 == 0 else 3
        if slot < 2:
            ref = cbuf.at[v, (z + (4 - d if recv else 0)) % 4, c]
        else:
            ref = cbuf.at[v, (z + (2 if recv else 4 - d)) % 4, c, pl.ds(0, 3), pl.ds((slot - 2) * 64, 64)]
        return remote(ref, ref, css.at[v, slot], crs.at[v, slot], near(2, d))

    def cacross(v, k, recv):
        core = 1 - c if recv else c
        if k < 3:
            ref = cbuf.at[v, (z + (0, 3, 1)[k]) % 4, core]
        else:
            ref = cbuf.at[v, (z + 2) % 4, core, pl.ds(0, 3), pl.ds((k - 3) * 64, 64)]
        return remote(ref, ref, dss.at[v, k], drs.at[v, k], partner)

    def ctx_start(v):
        cring(v, 0, False).start()
        cring(v, 1, False).start()
        cacross(v, 0, False).start()

    def ctx_forward(v):
        for slot in (0, 1):
            cring(v, slot, True).wait_recv()
            cring(v, slot + 2, False).start()
            cacross(v, 1 + slot, False).start()

    def ctx_finish(v):
        for slot in (2, 3):
            cring(v, slot, True).wait_recv()
            cacross(v, 1 + slot, False).start()

    def ctx_ready(v):
        for k in range(5):
            cacross(v, k, True).wait_recv()

    slab = z * 2 + c

    def owner(v, q):
        return (q // 4) * 8 + (q % 4) * 2 + v // 4

    def sixteen(v):
        return pl.ds(pl.multiple_of((v % 4) * 16, 16), 16)

    def send(v, q):
        return remote(part.at[v, pl.ds(pl.multiple_of(q * 16, 16), 16)], rbuf.at[x_hi, slab, sixteen(v)],
                      fss.at[v, q], frs.at[x_hi, slab], (row, owner(v, q)))

    def arrival(hi, t):
        return remote(rbuf.at[hi, t], rbuf.at[hi, t], fss.at[0, 0], frs.at[hi, t], (row, hi * 8 + t))

    p_copy = pltpu.make_async_copy(p_hbm, p2d, osem.at[2])
    p_copy.start()

    barrier = pltpu.get_barrier_semaphore()
    peers = [near(a, d) for a in range(3) for d in (1, 2, 3)] + [partner]
    for peer in peers:
        pl.semaphore_signal(barrier, inc=1, device_id=peer, device_id_type=MESH)

    @pl.when(jnp.logical_not(stays))
    def _():
        pl.semaphore_signal(barrier, inc=1, device_id=w1_to, device_id_type=MESH)
    for t in range(16):
        @pl.when(col != t)
        def _():
            pl.semaphore_signal(barrier, inc=1, device_id=(row, t), device_id_type=MESH)

    def prepare(lhs, wq, emb, res, mu):
        wp = lhs
        wp_copies = [
            pltpu.make_async_copy(wp_hbm.at[pl.ds(i * 192, 192)], wp.at[pl.ds(i * 192, 192)], lsem.at[i])
            for i in range(4)]
        for cp in wp_copies:
            cp.start()
        wq_copies = [pltpu.make_async_copy(wq_hbm.at[b // 3, b % 3], wq.at[b], wsem.at[b]) for b in range(9)]
        for cp in wq_copies:
            cp.start()

        pl.semaphore_wait(barrier, jnp.where(stays, len(peers) + 15, len(peers) + 16))
        cast_start(0)
        p_copy.wait()
        own_copies = [
            pltpu.make_async_copy(p2d.at[:, pl.ds(p * 256, 256)], buf.at[p, x, y, z, c], osem.at[3 + p])
            for p in range(3)]
        for cp in own_copies:
            cp.start()

        gain = bg[1:2, :]
        gain_lo, gain_hi = gain[:, :3072], gain[:, 3072:]
        bias = bg[0:1, :]

        lhs[ROW_C:ROW_C + 128, 0:3072] = jnp.zeros((128, 3072), BF16)
        lhs[ROW_R:ROW_R + 64, 3072:6144] = jnp.zeros((64, 3072), BF16)
        sbv, cbv = sb[...], cb[...]
        for t in range(8):
            sins, coss = [], []
            for u in (2 * t, 2 * t + 1):
                sav, cav = sa[u:u + 1, :], ca[u:u + 1, :]
                sins.append(sav * cbv + cav * sbv)
                coss.append(cav * cbv - sav * sbv)
            table = jnp.concatenate([jnp.concatenate(sins, 0), jnp.concatenate(coss, 0)], axis=1)
            mu[16 * t:16 * t + 16, :] = jnp.broadcast_to(
                jnp.sum(table, axis=1, keepdims=True) * (1.0 / 6144), (16, 128))
            lhs[ROW_C + 16 * t:ROW_C + 16 * t + 16, 3072:6144] = (table * gain_hi).astype(BF16)
            if t < 4:
                lhs[ROW_R + 16 * t:ROW_R + 16 * t + 16, 0:3072] = (table * gain_lo).astype(BF16)
        bias_c = (bias - jnp.mean(bias, axis=1, keepdims=True)) * gain
        tail_rows = lax.broadcasted_iota(jnp.int32, (48, 6144), 0)
        lhs[ROW_BIAS:ROW_BIAS + 48, :] = jnp.where(
            tail_rows == 0, bias_c, jnp.where(tail_rows == 1, gain, 0.0)).astype(BF16)

        for cp in wp_copies:
            cp.wait()
        for cp in own_copies:
            cp.wait()
        cast_wait(0)
        cast_start(1)

        def own_table(n):
            sav, cav = sa[pl.ds(n, 1), :], ca[pl.ds(n, 1), :]
            return jnp.concatenate([sav * cbv + cav * sbv, cav * cbv - sav * sbv], axis=1)

        t_row, t_col = own_table(row), own_table(col)
        pixels = p2d[...]
        total = jnp.zeros((64, 1), F32)
        for n in range(12):
            lo = n * 512
            e = jnp.dot(pixels, wp[0:768, lo:lo + 512], preferred_element_type=F32) + bias[:, lo:lo + 512]
            e = e.reshape(8, 8, 512)
            if n < 6:
                e = e + t_row[:, lo:lo + 512].reshape(8, 1, 512)
            else:
                e = e + t_col[:, lo - 3072:lo - 2560].reshape(1, 8, 512)
            e = e.reshape(64, 512)
            emb[:, lo:lo + 512] = e
            total = total + jnp.sum(e, axis=1, keepdims=True)
        mean = total * (1.0 / 6144)
        square = jnp.zeros((64, 1), F32)
        for n in range(12):
            d = emb[:, n * 512:n * 512 + 512] - mean
            square = square + jnp.sum(d * d, axis=1, keepdims=True)
        rstd = lax.rsqrt(square * (1.0 / 6144) + NORM_EPS)
        rs_wide = jnp.concatenate([jnp.broadcast_to(rstd, (64, 128)), jnp.zeros((64, 128), F32)], axis=0)
        rsown[...] = rs_wide.T[0:1, :]
        rs_own_copy = pltpu.make_async_copy(rsown, rsbuf.at[x, y, z, c], osem.at[1])
        rs_own_copy.start()
        rs_step(0)

        def center(i, carry):
            w = wp[pl.ds(pl.multiple_of(i * 48, 48), 48), :].astype(F32)
            w = (w - jnp.mean(w, axis=1, keepdims=True)) * gain
            lhs[pl.ds(pl.multiple_of(i * 48, 48), 48), :] = w.astype(BF16)
            return carry

        lax.fori_loop(0, 5, center, 0)
        rs_own_copy.wait()
        rs_wait(0)
        rs_step(1)
        lax.fori_loop(5, 11, center, 0)
        rs_wait(1)
        rs_step(2)
        cast_wait(1)
        start_phase()
        for p in range(3):
            across(p, 0, False).start()
        lax.fori_loop(11, 16, center, 0)
        for cp in wq_copies:
            cp.wait()

        def product(it, carry):
            pair = it // 3
            rows = pl.ds(pl.multiple_of((it % 3) * LHS_TILE, LHS_TILE), LHS_TILE)
            second = jnp.minimum(2 * pair + 1, 8)
            w = jnp.concatenate([wq[2 * pair], wq[second]], axis=1)
            res[pair, rows, :] = jnp.dot(lhs[rows, :], w, preferred_element_type=F32)

            @pl.when(it == 0)
            def _():
                rs_wait(2)
                rs_step(3)

            @pl.when(it == 5)
            def _():
                forward_phase()

            @pl.when(it == 10)
            def _():
                direct_phase()

            @pl.when(it == 14)
            def _():
                finish_phase()

                @pl.when(stays)
                def _():
                    w1_local().start()

                @pl.when(jnp.logical_not(stays))
                def _():
                    w1(False).start()
            return carry

        lax.fori_loop(0, 15, product, 0)

        mus = mu[...]
        for b in range(9):
            lanes = slice((b % 2) * 128, (b % 2) * 128 + 128)
            w = res[b // 2, 0:768, lanes]
            gsum = res[b // 2, ROW_GAIN:ROW_GAIN + 1, lanes]
            rp = res[b // 2, ROW_R:ROW_R + 64, lanes] - mus[:64] * gsum + res[b // 2, ROW_BIAS:ROW_BIAS + 1, lanes]
            cp = res[b // 2, ROW_C:ROW_C + 128, lanes] - mus * gsum
            if b < 6:
                w = w - jnp.mean(w, axis=1, keepdims=True)
                rp = rp - jnp.mean(rp, axis=1, keepdims=True)
                cp = cp - jnp.mean(cp, axis=1, keepdims=True)
            lanes = slice(b * 128, b * 128 + 128)
            wres[:, lanes] = w.astype(BF16)
            rpos[:, lanes] = rp
            cpos[:, lanes] = cp
        rs_wait(3)

        across_wait()

    pl.run_scoped(
        prepare,
        pltpu.VMEM((LHS_ROWS, 6144), BF16),
        pltpu.VMEM((9, 6144, 128), BF16),
        pltpu.VMEM((64, 6144), F32),
        pltpu.VMEM((5, LHS_ROWS, 256), F32),
        pltpu.VMEM((128, 128), F32),
    )

    def attend(tiles, feats, feats2, rwide, kall, vall, qall):
        def tile_copies(n, slot):
            return [
                pltpu.make_async_copy(buf.at[p, n // 4, n % 4], tiles.at[slot, p], tsem.at[slot, p])
                for p in range(3)]

        def tile_start(n, slot):
            for cp in tile_copies(n, slot):
                cp.start()

        def tile_wait(n, slot):
            for cp in tile_copies(n, slot):
                cp.wait()

        scale = math.log2(math.e) / math.sqrt(128.0)

        def project(n, slot, first, width):
            cx, cy = n // 4, n % 4
            p = jnp.concatenate([tiles[slot, q].reshape(512, 256) for q in range(3)], axis=1)
            yv = jnp.dot(p, wres[:, first:first + width], preferred_element_type=F32).reshape(8, 8, 8, width)
            r = cy * 2 + cx % 2
            rp = rpos[pl.ds(pl.multiple_of(r * 8, 8), 8), first:first + width]
            cp = cpos[pl.ds(pl.multiple_of((cx // 2) * 64, 64), 64), first:first + width]
            yv = yv + rp.reshape(1, 8, 1, width) + cp.reshape(8, 1, 8, width)
            return yv.reshape(512, width)

        def rstd_of(n):
            rows = rsbuf[n // 4, n % 4].reshape(8, 128)
            rst = jnp.concatenate([rows, jnp.zeros((120, 128), F32)], axis=0).T
            return jnp.concatenate([rst[0:64, q:q + 1] for q in range(8)], axis=0)

        def normed(yh, rcol, gain):
            var = jnp.mean(yh * yh, axis=1, keepdims=True)
            return yh * (rcol * lax.rsqrt(rcol * rcol * var + NORM_EPS)) * gain

        def both(n, ref, nxt, slot, dest):
            rwide[...] = jnp.broadcast_to(rstd_of(n), (512, 128))
            cx, cy = nxt // 4, nxt % 4
            r = cy * 2 + cx % 2
            rp = rpos[pl.ds(pl.multiple_of(r * 8, 8), 8), 384:1152].reshape(1, 8, 1, 768)

            def rows(t, carry):
                here = pl.ds(pl.multiple_of(t * 256, 256), 256)
                p = jnp.concatenate([tiles[slot, q, pl.ds(t * 2, 2)].reshape(256, 256) for q in range(3)], axis=1)
                yv = jnp.dot(p, wres[:, 384:1152], preferred_element_type=F32).reshape(4, 8, 8, 768)
                cp = cpos[pl.ds(pl.multiple_of((cx // 2) * 64 + t * 32, 32), 32), 384:1152]
                dest[here, :] = (yv + rp + cp.reshape(4, 1, 8, 768)).reshape(256, 768)
                at = pl.ds(pl.multiple_of(n * 512 + t * 256, 256), 256)
                rs = rwide[here, :]
                for h in range(3):
                    yk = ref[here, h * 128:h * 128 + 128]
                    kall[h, at, :] = normed(yk, rs, qk_gain[h, 1:2, :]).astype(BF16)
                    vall[h, at, :] = (ref[here, 384 + h * 128:512 + h * 128] * rs).astype(BF16)
                return carry

            lax.fori_loop(0, 2, rows, 0)

        def store_q(n, slot):
            @pl.when((n % 4 == y) & ((n // 4) % 2 == x_lo))
            def _():
                yq, rq = project(n, slot, 0, 384), rstd_of(n)
                for h in range(3):
                    qh = normed(yq[:, h * 128:h * 128 + 128], rq, qk_gain[h, 0:1, :] * scale).reshape(8, 8, 8, 128)
                    for t in range(4):
                        for i in range(8):
                            dst = (n // 8) * 512 + t * 128 + i * 16
                            qall[h, pl.ds(pl.multiple_of(dst, 16), 16), :] = (
                                qh[2 * t:2 * t + 2, i].reshape(16, 128).astype(BF16))

        tile_start(0, 0)
        tile_start(1, 1)
        tile_wait(0, 0)
        store_q(0, 0)
        feats[...] = project(0, 0, 384, 768)
        tile_start(2, 0)

        def fill(m, carry):
            n = 2 * m
            tile_wait(n + 1, 1)
            store_q(n + 1, 1)
            both(n, feats, n + 1, 1, feats2)

            @pl.when(m < 7)
            def _():
                tile_start(n + 3, 1)
                tile_wait(n + 2, 0)
                store_q(n + 2, 0)
            nxt = jnp.minimum(n + 2, 14)
            both(n + 1, feats2, nxt, 0, feats)

            @pl.when(m < 6)
            def _():
                tile_start(n + 4, 0)

            @pl.when(m == 5)
            def _():
                w1_wait()
                wx(False).start()
                wring_start(0)
            return carry

        lax.fori_loop(0, 8, fill, 0)

        ones = jnp.ones((8192, 128), BF16)

        def project_out(v):
            a = jnp.concatenate([cbuf[v, t // 2, t % 2, h] for h in range(3) for t in range(8)], axis=1)
            w = []
            for h in range(3):
                for t in range(8):
                    if h == 0:
                        w.append(wslab[t, 0, 0:128, :])
                    elif h == 2:
                        w.append(wslab[t, 1, 64:192, :])
                    else:
                        w.append(wslab[t, 0, 128:192, :])
                        w.append(wslab[t, 1, 0:64, :])
            rows = jnp.dot(a, jnp.concatenate(w, axis=0), preferred_element_type=F32).astype(BF16)
            part[v] = rows
            for q in range(8):
                @pl.when(owner(v, q) == col)
                def _():
                    rbuf[x_hi, slab, sixteen(v), :] = rows[q * 16:q * 16 + 16, :]

        def ship(v):
            for k in range(8):
                q = (x_hi + k // 4) % 2 * 4 + (z + k) % 4

                @pl.when(owner(v, q) != col)
                def _():
                    send(v, q).start()

        def unit(v, carry):
            at = pl.ds(pl.multiple_of(v * QT, QT), QT)
            scores = [
                lax.dot_general(qall[h, at, :], kall[h], (((1,), (1,)), ((), ())), preferred_element_type=F32)
                for h in range(3)]
            for h in range(3):
                p = jnp.exp2(scores[h] - jnp.max(scores[h], axis=1, keepdims=True)).astype(BF16)
                a = jnp.dot(p, jnp.concatenate([vall[h], ones], axis=1), preferred_element_type=F32)
                cbuf[v, z, c, h] = (a[:, :128] / a[:, 128:]).astype(BF16)

            @pl.when(v >= 2)
            def _():
                ctx_finish(v - 2)

            @pl.when(v >= 1)
            def _():
                ctx_forward(v - 1)
            ctx_start(v)

            @pl.when(v == 1)
            def _():
                wx(True).wait_recv()
                wring_start(1)
                wring_forward(0)

            @pl.when(v == 5)
            def _():
                wring_forward(1)
            return carry

        lax.fori_loop(0, 8, unit, 0)
        wring_finish(0)
        wring_finish(1)

        def tail_unit(v, carry):
            @pl.when(v == 2)
            def _():
                ctx_finish(6)

            @pl.when(v == 3)
            def _():
                ctx_forward(7)
                ship(2)

            @pl.when(v == 5)
            def _():
                ship(3)

            @pl.when(v == 6)
            def _():
                ctx_finish(7)
                ship(4)
                ship(5)
            ctx_ready(v)
            project_out(v)

            @pl.when((v < 2) | (v == 6))
            def _():
                ship(v)
            return carry

        lax.fori_loop(0, 8, tail_unit, 0)
        ship(7)

    pl.run_scoped(
        attend,
        pltpu.VMEM((2, 3, 4, 2, 64, 256), BF16),
        pltpu.VMEM((512, 768), F32),
        pltpu.VMEM((512, 768), F32),
        pltpu.VMEM((512, 128), F32),
        pltpu.VMEM((3, 8192, 128), BF16),
        pltpu.VMEM((3, 8192, 128), BF16),
        pltpu.VMEM((3, 1024, 128), BF16),
    )

    for t in range(8):
        for hi in range(2):
            @pl.when(hi * 8 + t != col)
            def _():
                arrival(hi, t).wait_recv()
        out[:, t * 768:t * 768 + 768] = (rbuf[0, t].astype(F32) + rbuf[1, t].astype(F32)).astype(BF16)

    for p in range(3):
        for ph in range(2):
            for d in (1, 2, 3):
                cast(p, ph, d, False).wait_send()
        for slot in range(6):
            ring(p, slot, False).wait_send()
        for k in range(5):
            across(p, k, False).wait_send()
    for step in range(4):
        for d in ((0,) if step == 0 else (1, 2, 3)):
            rs_copy(step, d, False).wait_send()

    @pl.when(jnp.logical_not(stays))
    def _():
        w1(False).wait_send()
    wx(False).wait_send()
    for which in range(2):
        for slot in range(6):
            wring(which, slot, False).wait_send()

    def left(v, carry):
        for slot in range(4):
            cring(v, slot, False).wait_send()
        for k in range(5):
            cacross(v, k, False).wait_send()
        for q in range(8):
            @pl.when(owner(v, q) != col)
            def _():
                send(v, q).wait_send()
        return carry

    lax.fori_loop(0, 8, left, 0)


def fused(bg, qk_gain, patches, w_patch, w_qkv, w_out):
    tables = [jnp.asarray(t) for t in trig_tables()]
    vm = pl.BlockSpec(memory_space=pltpu.VMEM)
    anym = pl.BlockSpec(memory_space=pl.ANY)
    dma = pltpu.SemaphoreType.DMA
    return pl.pallas_call(
        fused_kernel,
        out_shape=(
            jax.ShapeDtypeStruct((64, 6144), BF16),
            jax.ShapeDtypeStruct((3, 4, 4, 4, 2, 64, 256), BF16),
        ),
        in_specs=[vm] * 6 + [anym] * 4,
        out_specs=(vm, anym),
        scratch_shapes=[
            pltpu.VMEM((64, 768), BF16),
            pltpu.VMEM((4, 4, 4, 2, 1, 128), F32),
            pltpu.VMEM((1, 128), F32),
            pltpu.VMEM((768, 1152), BF16),
            pltpu.VMEM((64, 1152), F32),
            pltpu.VMEM((128, 1152), F32),
            pltpu.VMEM((8, 4, 2, 3, 128, 128), BF16),
            pltpu.VMEM((8, 2, 192, 768), BF16),
            pltpu.VMEM((8, 128, 768), BF16),
            pltpu.VMEM((2, 8, 64, 768), BF16),
            dma((3, 6)), dma((3, 6)), dma((3, 5)), dma((3, 5)),
            dma((4, 4)), dma((4, 4)), dma((4,)), dma((9,)), dma((6,)),
            dma, dma, dma, dma, dma((2, 6)), dma((2, 6)),
            dma((8, 4)), dma((8, 4)), dma((8, 5)), dma((8, 5)), dma((8, 8)), dma((2, 8)), dma((2, 3)),
            dma((3, 2, 4)), dma((3, 2, 4)),
        ],
        compiler_params=pltpu.CompilerParams(collective_id=0, has_side_effects=True, vmem_limit_bytes=VMEM_LIMIT),
        name="fused",
    )(bg, qk_gain, *tables, patches, w_patch, w_qkv, w_out)


def local(patches, w_patch, patch_bias, ln_gain, w_qkv, qk_gain, w_out):
    bg = jnp.stack([patch_bias, ln_gain]).astype(F32)
    out, _ = fused(
        bg, qk_gain.transpose(1, 0, 2), patches.reshape(64, 768), w_patch,
        w_qkv.transpose(1, 2, 0, 3), w_out.reshape(2, 192, 768))
    return out


def solution(mesh):
    return jax.shard_map(
        local,
        mesh=mesh,
        in_specs=(
            P("row", "col", None), P(), P(), P(),
            P(None, None, "col", None), P(None, "col", None), P("col", None, "row"),
        ),
        out_specs=P(("row", "col"), None),
        check_vma=False,
    )
```
